32 devices in a mesh: rep: 2 (over x), head: 4 (over z), seq: 4 (over y, core).
Axes of the slice: x: 2, y: 2, z: 4, core: 2. Of those that a mesh axis runs over, the one named last changes fastest.
Arguments:
- tokens: bfloat16 [128, 8192], P('rep'), parts along dimension 0
- w_query: bfloat16 [8192, 8192], replicated
- w_key: bfloat16 [8192, 1024], replicated
- w_value: bfloat16 [8192, 1024], replicated
- w_out: bfloat16 [8192, 8192], P(('head', 'seq'))
- k_cache: bfloat16 [128, 1024, 8, 128], P('rep', 'seq', 'head'), parts along dimension 0
- v_cache: bfloat16 [128, 1024, 8, 128], P('rep', 'seq', 'head'), parts along dimension 0
- positions: int32 [128], P('rep'), parts along dimension 0
Outputs:
- output 1: bfloat16 [128, 8192], P('rep'), parts along dimension 0
- output 2: bfloat16 [128, 1024, 8, 128], P('rep', 'seq', 'head'), parts along dimension 0
- output 3: bfloat16 [128, 1024, 8, 128], P('rep', 'seq', 'head'), parts along dimension 0
There are 2 independent parts. The reference program is written for one: setup_inputs(seed, part) draws one part's arguments, and reference() takes and returns one part's arrays. A program takes and returns all parts, laid end to end along the dimension named above; an argument that names none is the same for every part.
All inputs are finite; a program needn't handle non-finite values.
Results may differ from the reference program's by a relative error of at most 0.00554661.
Values are sent between devices in bfloat16 or wider.
A program may use at most 1 GiB of HBM per device.

```python
import math
import jax
import jax.numpy as jnp
from jax import lax

BATCH = 64
D_MODEL = 8192
N_HEADS = 64
N_KV = 8
HEAD_DIM = 128
SHARD_LEN = 256
SEQ_LEN = 1024
KEY_SCALE = math.sqrt(math.log(SHARD_LEN / 16))


def setup_inputs(seed: int = 0, part: int = 0) -> dict:
    base_key = jax.random.key(seed)
    part_key = jax.random.fold_in(base_key, part)
    weight_keys = jax.random.split(base_key, 4)
    part_keys = jax.random.split(part_key, 4)
    tokens = jax.random.normal(part_keys[0], (BATCH, D_MODEL), jnp.float32)
    w_query = jax.random.normal(weight_keys[0], (D_MODEL, N_HEADS * HEAD_DIM), jnp.float32) * D_MODEL ** -0.5
    w_key = jax.random.normal(weight_keys[1], (D_MODEL, N_KV * HEAD_DIM), jnp.float32) * (KEY_SCALE * D_MODEL ** -0.5)
    w_value = jax.random.normal(weight_keys[2], (D_MODEL, N_KV * HEAD_DIM), jnp.float32) * D_MODEL ** -0.5
    w_out = jax.random.normal(weight_keys[3], (N_HEADS * HEAD_DIM, D_MODEL), jnp.float32) * (N_HEADS * HEAD_DIM) ** -0.5
    k_cache = jax.random.normal(part_keys[1], (BATCH, SEQ_LEN, N_KV, HEAD_DIM), jnp.float32) * KEY_SCALE
    v_cache = jax.random.normal(part_keys[2], (BATCH, SEQ_LEN, N_KV, HEAD_DIM), jnp.float32)
    positions = jax.random.randint(part_keys[3], (BATCH,), 0, SEQ_LEN, jnp.int32)
    positions = positions.at[0].set(SEQ_LEN - 1)
    return {
        'tokens': tokens.astype(jnp.bfloat16),
        'w_query': w_query.astype(jnp.bfloat16),
        'w_key': w_key.astype(jnp.bfloat16),
        'w_value': w_value.astype(jnp.bfloat16),
        'w_out': w_out.astype(jnp.bfloat16),
        'k_cache': k_cache.astype(jnp.bfloat16),
        'v_cache': v_cache.astype(jnp.bfloat16),
        'positions': positions,
    }


def reference(tokens, w_query, w_key, w_value, w_out, k_cache, v_cache, positions):
    groups = N_HEADS // N_KV
    query = jnp.dot(tokens, w_query, preferred_element_type=jnp.float32).astype(jnp.bfloat16)
    new_key = jnp.dot(tokens, w_key, preferred_element_type=jnp.float32).astype(jnp.bfloat16)
    new_value = jnp.dot(tokens, w_value, preferred_element_type=jnp.float32).astype(jnp.bfloat16)
    query = query.reshape(BATCH, N_KV, groups, HEAD_DIM)
    new_key = new_key.reshape(BATCH, N_KV, HEAD_DIM)
    new_value = new_value.reshape(BATCH, N_KV, HEAD_DIM)
    slot_ids = jnp.arange(SEQ_LEN, dtype=jnp.int32)

    def one_row(row_inputs):
        q_row, key_row, value_row, k_rows, v_rows, pos_row = row_inputs
        is_slot = (slot_ids == pos_row)[:, None, None]
        k_new = jnp.where(is_slot, key_row[None], k_rows)
        v_new = jnp.where(is_slot, value_row[None], v_rows)
        scores = jnp.einsum('kgd,tkd->kgt', q_row.astype(jnp.float32), k_new.astype(jnp.float32)) * HEAD_DIM ** -0.5
        scores = jnp.where(slot_ids <= pos_row, scores, -jnp.inf)
        row_max = jnp.max(scores, axis=-1, keepdims=True)
        weights = jnp.exp(scores - row_max)
        row_sum = jnp.sum(weights, axis=-1, keepdims=True)
        mixed_sum = jnp.einsum('kgt,tkd->kgd', weights.astype(jnp.bfloat16).astype(jnp.float32), v_new.astype(jnp.float32))
        attn_row = (mixed_sum / row_sum).astype(jnp.bfloat16)
        return k_new, v_new, attn_row

    k_out, v_out, attn_rows = lax.map(one_row, (query, new_key, new_value, k_cache, v_cache, positions))
    attn_flat = attn_rows.reshape(BATCH, N_HEADS * HEAD_DIM)
    y_out = jnp.dot(attn_flat, w_out, preferred_element_type=jnp.float32).astype(jnp.bfloat16)
    return y_out, k_out, v_out
```

```python
import functools

import jax
import jax.numpy as jnp
from jax import lax
from jax.experimental import pallas as pl
from jax.experimental.pallas import tpu as pltpu
from jax.sharding import PartitionSpec as P

MESH = pl.DeviceIdType.MESH
ANY = pl.BlockSpec(memory_space=pl.ANY)
VMEM = pl.BlockSpec(memory_space=pltpu.VMEM)
SMEM = pl.BlockSpec(memory_space=pltpu.SMEM)
N_SEQ = 4
N_HEAD = 4
LANES = 128
F32 = jnp.float32
BF16 = jnp.bfloat16


def entry_barrier(axes):
    sem = pltpu.get_barrier_semaphore()
    count = 0
    for axis, size in axes:
        me = lax.axis_index(axis)
        for step in range(1, size):
            pl.semaphore_signal(sem, inc=1, device_id={axis: lax.rem(me + step, size)}, device_id_type=MESH)
            count += 1
    return lambda: pl.semaphore_wait(sem, count)


def project_kernel(n_chunk, tok_hbm, wq_hbm, wk_hbm, wv_hbm, out, tok, wq, wkv, acc, acc_kv, stage, load_sem, send_sem, recv_sem):
    head, seq = lax.axis_index('head'), lax.axis_index('seq')
    q_cols, depth = wq.shape[2], wq.shape[1]
    n_q = q_cols // LANES
    batch = tok.shape[0]
    wait_peers = entry_barrier((('seq', N_SEQ),))

    q_at = pl.multiple_of((head * N_SEQ + seq) * q_cols, q_cols)
    kv_at = pl.multiple_of((head * 2 + lax.rem(seq, 2)) * LANES, LANES)

    def tok_copy(c):
        return pltpu.make_async_copy(tok_hbm.at[:, pl.ds(c * depth, depth)], tok.at[:, pl.ds(c * depth, depth)], load_sem.at[0, c])

    def q_copy(c):
        return pltpu.make_async_copy(wq_hbm.at[pl.ds(c * depth, depth), pl.ds(q_at, q_cols)], wq.at[c], load_sem.at[1, c])

    def kv_copy(src, c):
        return pltpu.make_async_copy(src.at[pl.ds(c * depth, depth), pl.ds(kv_at, LANES)], wkv.at[c], load_sem.at[2, c])

    for c in range(n_chunk):
        tok_copy(c).start()
        q_copy(c).start()

        @pl.when(seq < 2)
        def _():
            kv_copy(wk_hbm, c).start()

        @pl.when(seq >= 2)
        def _():
            kv_copy(wv_hbm, c).start()

    for c in range(n_chunk):
        tok_copy(c).wait()
        q_copy(c).wait()
        kv_copy(wk_hbm, c).wait()
        x = tok[:, c * depth:(c + 1) * depth]
        q_part = jnp.dot(x, wq[c], preferred_element_type=F32)
        kv_part = jnp.dot(x, wkv[c], preferred_element_type=F32)
        if c == 0:
            acc[...] = q_part
            acc_kv[...] = kv_part
        else:
            acc[...] += q_part
            acc_kv[...] += kv_part
    for i in range(n_q):
        stage[i] = acc[:, i * LANES:(i + 1) * LANES].astype(BF16)
    stage[n_q] = acc_kv[...].astype(BF16)

    wait_peers()
    copies = []
    for step in range(1, N_SEQ):
        copies.append(pltpu.make_async_remote_copy(
            src_ref=stage, dst_ref=out.at[seq], send_sem=send_sem.at[step - 1], recv_sem=recv_sem.at[step - 1],
            device_id={'seq': lax.rem(seq + step, N_SEQ)}, device_id_type=MESH))
        copies[-1].start()
    out[seq] = stage[...]
    for copy in copies:
        copy.wait()


def project(tokens, w_query, w_key, w_value):
    batch, d_model = tokens.shape
    q_cols = w_query.shape[1] // (N_HEAD * N_SEQ)
    n_chunk = 8
    depth = d_model // n_chunk
    n_q = q_cols // LANES
    return pl.pallas_call(
        functools.partial(project_kernel, n_chunk),
        out_shape=jax.ShapeDtypeStruct((N_SEQ, n_q + 1, batch, LANES), BF16),
        in_specs=[ANY] * 4,
        out_specs=VMEM,
        scratch_shapes=[
            pltpu.VMEM((batch, d_model), BF16),
            pltpu.VMEM((n_chunk, depth, q_cols), BF16),
            pltpu.VMEM((n_chunk, depth, LANES), BF16),
            pltpu.VMEM((batch, q_cols), F32),
            pltpu.VMEM((batch, LANES), F32),
            pltpu.VMEM((n_q + 1, batch, LANES), BF16),
            pltpu.SemaphoreType.DMA((3, n_chunk)),
            pltpu.SemaphoreType.DMA((N_SEQ - 1,)),
            pltpu.SemaphoreType.DMA((N_SEQ - 1,)),
        ],
        compiler_params=pltpu.CompilerParams(collective_id=0, has_side_effects=True),
        name='project',
    )(tokens, w_query, w_key, w_value)


def attend_kernel(n_chunk, shard_len, pos_ref, qkv_ref, k_hbm, v_hbm, k_out, v_out, mix_out, ml_out,
                  kbuf, vbuf, qf, kvf, load_sem, store_sem):
    batch, rows = kbuf.shape[0], kbuf.shape[1]
    n_q = qkv_ref.shape[1] - 1
    n_rows = N_SEQ * n_q
    per = batch // n_chunk
    start = lax.axis_index('seq') * shard_len

    def load(hbm, buf, which, c):
        return pltpu.make_async_copy(hbm.at[pl.ds(c * per, per)], buf.at[pl.ds(c * per, per)], load_sem.at[which, c])

    def store(hbm, buf, which, c):
        return pltpu.make_async_copy(buf.at[pl.ds(c * per, per)], hbm.at[pl.ds(c * per, per)], store_sem.at[which, c])

    for c in range(n_chunk):
        load(k_hbm, kbuf, 0, c).start()
        load(v_hbm, vbuf, 1, c).start()

    for s in range(N_SEQ):
        for i in range(n_q):
            at = (s * n_q + i) * batch
            qf[at:at + batch, :] = qkv_ref[s, i].astype(F32)
        kvf[s * batch:(s + 1) * batch, :] = qkv_ref[s, n_q].astype(F32)

    col = lax.broadcasted_iota(jnp.int32, (n_rows, rows), 1)
    row = lax.broadcasted_iota(jnp.int32, (n_rows, rows), 0)
    slot = jnp.where((col & 1) == row // (n_rows // 2), col >> 1, jnp.int32(1 << 30))
    win_row = lax.broadcasted_iota(jnp.int32, (16, LANES), 0)
    win_odd = (win_row & 1) == 1
    win_slot = win_row >> 1
    lane = lax.broadcasted_iota(jnp.int32, (n_rows, LANES), 1)

    def chunk(c, ml):
        load(k_hbm, kbuf, 0, c).wait()
        load(v_hbm, vbuf, 1, c).wait()
        for j in range(per):
            b = c * per + j
            pos = pos_ref[b] - start
            inside = jnp.logical_and(pos >= 0, pos < shard_len)
            slot_at = jnp.clip(pos, 0, shard_len - 1)
            base = pl.multiple_of((slot_at // 8) * 16, 16)
            hit = win_slot == jnp.where(inside, lax.rem(slot_at, 8), -1)
            for buf, first in ((kbuf, 0), (vbuf, 2)):
                new = jnp.where(win_odd, kvf[pl.ds((first + 1) * batch + b, 1), :], kvf[pl.ds(first * batch + b, 1), :])
                old = buf[b, pl.ds(base, 16), :]
                buf[b, pl.ds(base, 16), :] = jnp.where(hit, new.astype(BF16), old)
        for j in range(per):
            b = c * per + j
            limit = pos_ref[b] - start
            q = qf[pl.ds(b, n_rows, stride=batch), :].astype(BF16)
            s = lax.dot_general(q, kbuf[b], (((1,), (1,)), ((), ())), preferred_element_type=F32) * LANES ** -0.5
            s = jnp.where(slot <= limit, s, -jnp.inf)
            m = jnp.max(s, axis=1, keepdims=True)
            safe = jnp.where(m == -jnp.inf, 0.0, m)
            w = jnp.exp(s - safe)
            l = jnp.sum(w, axis=1, keepdims=True)
            mix = jnp.dot(w.astype(BF16), vbuf[b], preferred_element_type=F32)
            mix_out[pl.ds(b, n_rows, stride=batch), :] = mix
            ml = jnp.where(lane == b, m, jnp.where(lane == batch + b, l, ml))
        store(k_out, kbuf, 0, c).start()
        store(v_out, vbuf, 1, c).start()
        return ml

    ml = lax.fori_loop(0, n_chunk, chunk, jnp.zeros((n_rows, LANES), F32))
    ml_out[...] = jnp.zeros_like(ml_out)
    for s in range(N_SEQ):
        ml_out[s, 0:n_q, :] = ml[s * n_q:(s + 1) * n_q, :]
    for c in range(n_chunk):
        store(k_out, kbuf, 0, c).wait()
        store(v_out, vbuf, 1, c).wait()


def attend(positions, qkv, k_cache, v_cache, shard_len):
    batch, rows, _ = k_cache.shape
    n_rows = N_SEQ * (qkv.shape[1] - 1)
    n_chunk = 8
    cache = jax.ShapeDtypeStruct(k_cache.shape, BF16)
    return pl.pallas_call(
        functools.partial(attend_kernel, n_chunk, shard_len),
        out_shape=[cache, cache, jax.ShapeDtypeStruct((n_rows * batch, LANES), F32), jax.ShapeDtypeStruct((N_SEQ, 8, LANES), F32)],
        in_specs=[SMEM, VMEM, ANY, ANY],
        out_specs=[ANY, ANY, VMEM, VMEM],
        scratch_shapes=[
            pltpu.VMEM((batch, rows, LANES), BF16),
            pltpu.VMEM((batch, rows, LANES), BF16),
            pltpu.VMEM((n_rows * batch, LANES), F32),
            pltpu.VMEM((N_SEQ * batch, LANES), F32),
            pltpu.SemaphoreType.DMA((2, n_chunk)),
            pltpu.SemaphoreType.DMA((2, n_chunk)),
        ],
        name='attend',
    )(positions, qkv, k_cache, v_cache)


def output_kernel(mix, ml, wo_hbm, y, wo, mix_in, ml_in, attn, give, own, core_in, y_in, z_in,
                  wo_sem, a_send, a_recv, m_send, m_recv, c_send, c_recv, y_send, y_recv, z_send, z_recv,
                  gz_send, gz_recv, gy_send, gy_recv, gc_send, gc_recv):
    head, seq = lax.axis_index('head'), lax.axis_index('seq')
    side, core = seq // 2, lax.rem(seq, 2)
    partner = side * 2 + (1 - core)
    across = (1 - side) * 2 + core
    n_q, batch = mix_in.shape[1], mix_in.shape[2]
    width = own.shape[2]
    wait_peers = entry_barrier((('seq', N_SEQ), ('head', N_HEAD)))

    def place(k):
        half = (1 - core) if k < 8 else core
        quarter = (1 - side) if (k % 8) < 4 else side
        z = lax.rem(head + 2 + k % 4, N_HEAD)
        return half, quarter, z

    def column(half, quarter, z):
        return pl.multiple_of(((half * 2 + quarter) * N_HEAD + z) * width, width)

    def wo_copy(k):
        return pltpu.make_async_copy(wo_hbm.at[:, pl.ds(column(*place(k)), width)], wo.at[k], wo_sem.at[k])

    for k in range(16):
        wo_copy(k).start()

    def remote(src, dst, send, recv, device):
        return pltpu.make_async_remote_copy(src_ref=src, dst_ref=dst, send_sem=send, recv_sem=recv, device_id=device, device_id_type=MESH)

    wait_peers()
    a_copies = []
    for step in range(1, N_SEQ):
        to = lax.rem(seq + step, N_SEQ)
        a_copies.append(remote(ml.at[to], ml_in.at[step - 1], m_send.at[step - 1], m_recv.at[step - 1], {'seq': to}))
        a_copies.append(remote(mix.at[pl.ds(to * n_q, n_q)], mix_in.at[step - 1], a_send.at[step - 1], a_recv.at[step - 1], {'seq': to}))
    for copy in a_copies:
        copy.start()
    for copy in a_copies:
        copy.wait()

    parts = [ml[seq]] + [ml_in[i] for i in range(N_SEQ - 1)]
    top = functools.reduce(jnp.maximum, parts)
    scales = [jnp.exp(p - top) for p in parts]
    total = functools.reduce(jnp.add, [pltpu.roll(p, LANES - batch, 1) * e for p, e in zip(parts, scales)])
    scales = [e / total for e in scales]
    table = jnp.concatenate(scales + [jnp.zeros((LANES - 8 * N_SEQ, LANES), F32)], axis=0).T
    for i in range(n_q):
        acc = mix[seq * n_q + i] * table[0:batch, i:i + 1]
        for s in range(1, N_SEQ):
            acc += mix_in[s - 1, i] * table[0:batch, s * 8 + i:s * 8 + i + 1]
        attn[:, i * LANES:(i + 1) * LANES] = acc.astype(BF16)

    def partial(k):
        wo_copy(k).wait()
        return jnp.dot(attn[...], wo[k], preferred_element_type=F32)

    c_copies = []
    for k in range(8):
        give[k] = partial(k)
        c_copies.append(remote(give.at[k], core_in.at[k], c_send.at[k], c_recv.at[k], {'seq': partner}))
        c_copies[-1].start()
    y_copies = []
    for k in range(4):
        value = partial(8 + k)
        c_copies[k].wait_recv()
        own[k] = value + core_in[k]
        y_copies.append(remote(own.at[k], y_in.at[k], y_send.at[k], y_recv.at[k], {'seq': across}))
        y_copies[-1].start()
    for k in range(4):
        own[4 + k] = partial(12 + k)
    z_copies = []
    for k in range(4):
        c_copies[4 + k].wait_recv()
        y_copies[k].wait_recv()
        own[4 + k] = own[4 + k] + core_in[4 + k] + y_in[k]
        step = (2 + k) % 4
        if step:
            z_copies.append(remote(own.at[4 + k], z_in.at[step - 1], z_send.at[step - 1], z_recv.at[step - 1],
                                   {'head': lax.rem(head + step, N_HEAD)}))
            z_copies[-1].start()
        else:
            mine = 4 + k
    for copy in z_copies:
        copy.wait_recv()
    here = column(core, side, head)
    y[:, pl.ds(here, width)] = (own[mine] + z_in[0] + z_in[1] + z_in[2]).astype(BF16)

    def spread(half, quarter, z, send, recv, device):
        at = y.at[:, pl.ds(column(half, quarter, z), width)]
        return remote(at, at, send, recv, device)

    sends = []

    def go(copy):
        copy.start()
        sends.append(copy)

    gz, gy, gc = {}, {}, {}
    for step in (2, 1, 3):
        gz[step] = spread(core, side, head, gz_send.at[step - 1], gz_recv.at[step - 1], {'head': lax.rem(head + step, N_HEAD)})
        go(gz[step])
    gy[0] = spread(core, side, head, gy_send.at[0], gy_recv.at[0], {'seq': across})
    gc[0] = spread(core, side, head, gc_send.at[0], gc_recv.at[0], {'seq': partner})
    go(gy[0])
    go(gc[0])
    for step in (1, 3, 2):
        source = lax.rem(head + N_HEAD - step, N_HEAD)
        gz[step].wait_recv()
        gy[step] = spread(core, side, source, gy_send.at[step], gy_recv.at[step], {'seq': across})
        gc[step] = spread(core, side, source, gc_send.at[step], gc_recv.at[step], {'seq': partner})
        go(gy[step])
        go(gc[step])
    for step in (0, 1, 3, 2):
        source = lax.rem(head + N_HEAD - step, N_HEAD)
        gy[step].wait_recv()
        gc[4 + step] = spread(core, 1 - side, source, gc_send.at[4 + step], gc_recv.at[4 + step], {'seq': partner})
        go(gc[4 + step])
    for step in range(8):
        gc[step].wait_recv()
    for copy in a_copies[:0] + c_copies + y_copies + z_copies + sends:
        copy.wait_send()


def output(mix, ml, w_out):
    rows, d_out = w_out.shape
    n_q = rows // LANES
    batch = mix.shape[0] // (N_SEQ * n_q)
    width = d_out // 16
    dma = pltpu.SemaphoreType.DMA
    return pl.pallas_call(
        output_kernel,
        out_shape=jax.ShapeDtypeStruct((batch, d_out), BF16),
        in_specs=[VMEM, VMEM, ANY],
        out_specs=VMEM,
        scratch_shapes=[
            pltpu.VMEM((16, rows, width), BF16),
            pltpu.VMEM((3, n_q, batch, LANES), F32),
            pltpu.VMEM((3, 8, LANES), F32),
            pltpu.VMEM((batch, rows), BF16),
            pltpu.VMEM((8, batch, width), F32),
            pltpu.VMEM((8, batch, width), F32),
            pltpu.VMEM((8, batch, width), F32),
            pltpu.VMEM((4, batch, width), F32),
            pltpu.VMEM((3, batch, width), F32),
            dma((16,)),
            dma((3,)), dma((3,)), dma((3,)), dma((3,)),
            dma((8,)), dma((8,)), dma((4,)), dma((4,)), dma((3,)), dma((3,)),
            dma((3,)), dma((3,)), dma((4,)), dma((4,)), dma((8,)), dma((8,)),
        ],
        compiler_params=pltpu.CompilerParams(collective_id=1, has_side_effects=True),
        name='output',
    )(mix.reshape(N_SEQ * n_q, batch, LANES), ml, w_out)


def solution(mesh):
    cache_spec = P('rep', 'seq', 'head', None)

    def local_step(tokens, w_query, w_key, w_value, w_out, k_cache, v_cache, positions):
        batch, shard_len, kv_local, head_dim = k_cache.shape
        flat = (batch, shard_len * kv_local, head_dim)
        qkv = project(tokens, w_query, w_key, w_value)
        k_new, v_new, mix, ml = attend(positions, qkv, k_cache.reshape(flat), v_cache.reshape(flat), shard_len)
        y = output(mix, ml, w_out)
        return y, k_new.reshape(k_cache.shape), v_new.reshape(v_cache.shape)

    return jax.shard_map(
        local_step,
        mesh=mesh,
        in_specs=(P('rep', None), P(), P(), P(), P(('head', 'seq'), None), cache_spec, cache_spec, P('rep')),
        out_specs=(P('rep', None), cache_spec, cache_spec),
        check_vma=False,
    )
```

```python
import functools

import jax
import jax.numpy as jnp
from jax import lax
from jax.experimental import pallas as pl
from jax.experimental.pallas import tpu as pltpu
from jax.sharding import PartitionSpec as P

MESH = pl.DeviceIdType.MESH
HBM = pl.BlockSpec(memory_space=pltpu.HBM)
VMEM = pl.BlockSpec(memory_space=pltpu.VMEM)
SMEM = pl.BlockSpec(memory_space=pltpu.SMEM)
N_SEQ = 4
N_HEAD = 4
LANES = 128
F32 = jnp.float32
BF16 = jnp.bfloat16


def in_hbm(x):
    return pltpu.with_memory_space_constraint(x, pltpu.HBM)


def entry_barrier(axes):
    sem = pltpu.get_barrier_semaphore()
    count = 0
    for axis, size in axes:
        me = lax.axis_index(axis)
        for step in range(1, size):
            pl.semaphore_signal(sem, inc=1, device_id={axis: lax.rem(me + step, size)}, device_id_type=MESH)
            count += 1
    return lambda: pl.semaphore_wait(sem, count)


def project_kernel(n_chunk, ahead, tok_hbm, wq_hbm, wk_hbm, wv_hbm, k_hbm, v_hbm, out, kbuf, vbuf, tok, wq, wkv, acc, acc_kv, stage,
                   load_sem, cache_sem, send_sem, recv_sem):
    head, seq = lax.axis_index('head'), lax.axis_index('seq')
    q_cols, depth = wq.shape[2], wq.shape[1]
    n_q = q_cols // LANES
    batch = tok.shape[0]
    wait_peers = entry_barrier((('seq', N_SEQ),))

    q_at = pl.multiple_of((head * N_SEQ + seq) * q_cols, q_cols)
    kv_at = pl.multiple_of((head * 2 + lax.rem(seq, 2)) * LANES, LANES)

    def tok_copy(c):
        return pltpu.make_async_copy(tok_hbm.at[:, pl.ds(c * depth, depth)], tok.at[:, pl.ds(c * depth, depth)], load_sem.at[0, c])

    def q_copy(c):
        return pltpu.make_async_copy(wq_hbm.at[pl.ds(c * depth, depth), pl.ds(q_at, q_cols)], wq.at[c], load_sem.at[1, c])

    def kv_copy(src, c):
        return pltpu.make_async_copy(src.at[pl.ds(c * depth, depth), pl.ds(kv_at, LANES)], wkv.at[c], load_sem.at[2, c])

    def start(c):
        tok_copy(c).start()
        q_copy(c).start()

        @pl.when(seq < 2)
        def _():
            kv_copy(wk_hbm, c).start()

        @pl.when(seq >= 2)
        def _():
            kv_copy(wv_hbm, c).start()

    caches = []
    for g in range(8):
        span = pl.ds(g * (batch // 8), batch // 8)
        caches.append(pltpu.make_async_copy(k_hbm.at[span], kbuf.at[span], cache_sem.at[0, g]))
        caches.append(pltpu.make_async_copy(v_hbm.at[span], vbuf.at[span], cache_sem.at[1, g]))
    started = 0

    for c in range(ahead):
        start(c)
    for c in range(n_chunk):
        if c + ahead < n_chunk:
            start(c + ahead)
        else:
            for copy in caches[started:started + 4]:
                copy.start()
            started += 4
        tok_copy(c).wait()
        q_copy(c).wait()
        kv_copy(wk_hbm, c).wait()
        x = tok[:, c * depth:(c + 1) * depth]
        q_part = jnp.dot(x, wq[c], preferred_element_type=F32)
        kv_part = jnp.dot(x, wkv[c], preferred_element_type=F32)
        if c == 0:
            acc[...] = q_part
            acc_kv[...] = kv_part
        else:
            acc[...] += q_part
            acc_kv[...] += kv_part
    for i in range(n_q):
        stage[i] = acc[:, i * LANES:(i + 1) * LANES].astype(BF16)
    stage[n_q] = acc_kv[...].astype(BF16)

    wait_peers()
    copies = []
    for step in range(1, N_SEQ):
        copies.append(pltpu.make_async_remote_copy(
            src_ref=stage, dst_ref=out.at[seq], send_sem=send_sem.at[step - 1], recv_sem=recv_sem.at[step - 1],
            device_id={'seq': lax.rem(seq + step, N_SEQ)}, device_id_type=MESH))
        copies[-1].start()
    out[seq] = stage[...]
    for copy in copies:
        copy.wait()
    for copy in caches:
        copy.wait()


def project(tokens, w_query, w_key, w_value, k_cache, v_cache):
    batch, d_model = tokens.shape
    q_cols = w_query.shape[1] // (N_HEAD * N_SEQ)
    n_chunk = 8
    depth = d_model // n_chunk
    n_q = q_cols // LANES
    return pl.pallas_call(
        functools.partial(project_kernel, n_chunk, 4),
        out_shape=[pltpu.VMEM((N_SEQ, n_q + 1, batch, LANES), BF16), pltpu.VMEM(k_cache.shape, BF16), pltpu.VMEM(k_cache.shape, BF16)],
        in_specs=[HBM] * 6,
        out_specs=[VMEM] * 3,
        scratch_shapes=[
            pltpu.VMEM((batch, d_model), BF16),
            pltpu.VMEM((n_chunk, depth, q_cols), BF16),
            pltpu.VMEM((n_chunk, depth, LANES), BF16),
            pltpu.VMEM((batch, q_cols), F32),
            pltpu.VMEM((batch, LANES), F32),
            pltpu.VMEM((n_q + 1, batch, LANES), BF16),
            pltpu.SemaphoreType.DMA((3, n_chunk)),
            pltpu.SemaphoreType.DMA((2, 8)),
            pltpu.SemaphoreType.DMA((N_SEQ - 1,)),
            pltpu.SemaphoreType.DMA((N_SEQ - 1,)),
        ],
        compiler_params=pltpu.CompilerParams(collective_id=0, has_side_effects=True, vmem_limit_bytes=18 * 2**20),
        name='project',
    )(*map(in_hbm, (tokens, w_query, w_key, w_value, k_cache, v_cache)))


def attend_kernel(n_chunk, shard_len, pos_ref, qkv_ref, k_in, v_in, k_out, v_out, mix_out, ml_out, kbuf, vbuf,
                  qf, kvf, store_sem):
    batch, rows = kbuf.shape[0], kbuf.shape[1]
    n_q = qkv_ref.shape[1] - 1
    n_rows = N_SEQ * n_q
    per = batch // n_chunk
    start = lax.axis_index('seq') * shard_len

    def store(hbm, buf, which, c):
        return pltpu.make_async_copy(buf.at[pl.ds(c * per, per)], hbm.at[pl.ds(c * per, per)], store_sem.at[which, c])

    for s in range(N_SEQ):
        for i in range(n_q):
            at = (s * n_q + i) * batch
            qf[at:at + batch, :] = qkv_ref[s, i].astype(F32)
        kvf[s * batch:(s + 1) * batch, :] = qkv_ref[s, n_q].astype(F32)

    col = lax.broadcasted_iota(jnp.int32, (n_rows, rows), 1)
    row = lax.broadcasted_iota(jnp.int32, (n_rows, rows), 0)
    slot = jnp.where((col & 1) == row // (n_rows // 2), col >> 1, jnp.int32(1 << 30))
    win_row = lax.broadcasted_iota(jnp.int32, (16, LANES), 0)
    win_odd = (win_row & 1) == 1
    win_slot = win_row >> 1
    lane = lax.broadcasted_iota(jnp.int32, (n_rows, LANES), 1)

    def chunk(c, ml):
        for j in range(per):
            b = c * per + j
            pos = pos_ref[b] - start
            inside = jnp.logical_and(pos >= 0, pos < shard_len)
            slot_at = jnp.clip(pos, 0, shard_len - 1)
            base = pl.multiple_of((slot_at // 8) * 16, 16)
            hit = win_slot == jnp.where(inside, lax.rem(slot_at, 8), -1)
            for buf, first in ((kbuf, 0), (vbuf, 2)):
                new = jnp.where(win_odd, kvf[pl.ds((first + 1) * batch + b, 1), :], kvf[pl.ds(first * batch + b, 1), :])
                old = buf[b, pl.ds(base, 16), :]
                buf[b, pl.ds(base, 16), :] = jnp.where(hit, new.astype(BF16), old)
        store(k_out, kbuf, 0, c).start()
        store(v_out, vbuf, 1, c).start()
        for j in range(per):
            b = c * per + j
            limit = pos_ref[b] - start
            q = qf[pl.ds(b, n_rows, stride=batch), :].astype(BF16)
            s = lax.dot_general(q, kbuf[b], (((1,), (1,)), ((), ())), preferred_element_type=F32) * LANES ** -0.5
            s = jnp.where(slot <= limit, s, -jnp.inf)
            m = jnp.max(s, axis=1, keepdims=True)
            safe = jnp.where(m == -jnp.inf, 0.0, m)
            w = jnp.exp(s - safe)
            l = jnp.sum(w, axis=1, keepdims=True)
            mix = jnp.dot(w.astype(BF16), vbuf[b], preferred_element_type=F32)
            mix_out[pl.ds(b, n_rows, stride=batch), :] = mix
            ml = jnp.where(lane == b, m, jnp.where(lane == batch + b, l, ml))
        return ml

    ml = lax.fori_loop(0, n_chunk, chunk, jnp.zeros((n_rows, LANES), F32))
    ml_out[...] = jnp.zeros_like(ml_out)
    for s in range(N_SEQ):
        ml_out[s, 0:n_q, :] = ml[s * n_q:(s + 1) * n_q, :]
    for c in range(n_chunk):
        store(k_out, kbuf, 0, c).wait()
        store(v_out, vbuf, 1, c).wait()


def attend(positions, qkv, k_cache, v_cache, shard_len):
    batch, rows, _ = k_cache.shape
    n_rows = N_SEQ * (qkv.shape[1] - 1)
    n_chunk = 8
    cache = pltpu.HBM(k_cache.shape, BF16)
    held = pltpu.VMEM(k_cache.shape, BF16)
    return pl.pallas_call(
        functools.partial(attend_kernel, n_chunk, shard_len),
        out_shape=[cache, cache, pltpu.VMEM((n_rows * batch, LANES), F32), pltpu.VMEM((N_SEQ, 8, LANES), F32), held, held],
        in_specs=[SMEM, VMEM, VMEM, VMEM],
        out_specs=[HBM, HBM, VMEM, VMEM, VMEM, VMEM],
        input_output_aliases={2: 4, 3: 5},
        scratch_shapes=[
            pltpu.VMEM((n_rows * batch, LANES), F32),
            pltpu.VMEM((N_SEQ * batch, LANES), F32),
            pltpu.SemaphoreType.DMA((2, n_chunk)),
        ],
        compiler_params=pltpu.CompilerParams(vmem_limit_bytes=6 * 2**20),
        name='attend',
    )(positions, qkv, k_cache, v_cache)


def output_kernel(mix, ml, wo_hbm, y, wo, mix_in, ml_in, attn, give, own, core_in, y_in, z_in,
                  wo_sem, a_send, a_recv, m_send, m_recv, c_send, c_recv, y_send, y_recv, z_send, z_recv,
                  gz_send, gz_recv, gy_send, gy_recv, gc_send, gc_recv):
    head, seq = lax.axis_index('head'), lax.axis_index('seq')
    side, core = seq // 2, lax.rem(seq, 2)
    partner = side * 2 + (1 - core)
    across = (1 - side) * 2 + core
    n_q, batch = mix_in.shape[1], mix_in.shape[2]
    width = own.shape[2]
    wait_peers = entry_barrier((('seq', N_SEQ), ('head', N_HEAD)))

    def place(k):
        half = (1 - core) if k < 8 else core
        quarter = (1 - side) if (k % 8) < 4 else side
        z = lax.rem(head + 2 + k % 4, N_HEAD)
        return half, quarter, z

    def column(half, quarter, z):
        return pl.multiple_of(((half * 2 + quarter) * N_HEAD + z) * width, width)

    def wo_copy(k):
        return pltpu.make_async_copy(wo_hbm.at[:, pl.ds(column(*place(k)), width)], wo.at[k], wo_sem.at[k])

    for k in range(16):
        wo_copy(k).start()

    def remote(src, dst, send, recv, device):
        return pltpu.make_async_remote_copy(src_ref=src, dst_ref=dst, send_sem=send, recv_sem=recv, device_id=device, device_id_type=MESH)

    wait_peers()
    a_copies = []
    for step in range(1, N_SEQ):
        to = lax.rem(seq + step, N_SEQ)
        a_copies.append(remote(ml.at[to], ml_in.at[step - 1], m_send.at[step - 1], m_recv.at[step - 1], {'seq': to}))
        a_copies.append(remote(mix.at[pl.ds(to * n_q, n_q)], mix_in.at[step - 1], a_send.at[step - 1], a_recv.at[step - 1], {'seq': to}))
    for copy in a_copies:
        copy.start()
    for copy in a_copies:
        copy.wait()

    parts = [ml[seq]] + [ml_in[i] for i in range(N_SEQ - 1)]
    top = functools.reduce(jnp.maximum, parts)
    scales = [jnp.exp(p - top) for p in parts]
    total = functools.reduce(jnp.add, [pltpu.roll(p, LANES - batch, 1) * e for p, e in zip(parts, scales)])
    scales = [e / total for e in scales]
    table = jnp.concatenate(scales + [jnp.zeros((LANES - 8 * N_SEQ, LANES), F32)], axis=0).T
    for i in range(n_q):
        acc = mix[seq * n_q + i] * table[0:batch, i:i + 1]
        for s in range(1, N_SEQ):
            acc += mix_in[s - 1, i] * table[0:batch, s * 8 + i:s * 8 + i + 1]
        attn[:, i * LANES:(i + 1) * LANES] = acc.astype(BF16)

    def partial(k):
        wo_copy(k).wait()
        return jnp.dot(attn[...], wo[k], preferred_element_type=F32)

    c_copies = []
    for k in range(8):
        give[k] = partial(k)
        c_copies.append(remote(give.at[k], core_in.at[k], c_send.at[k], c_recv.at[k], {'seq': partner}))
        c_copies[-1].start()
    y_copies = []
    for k in range(4):
        value = partial(8 + k)
        c_copies[k].wait_recv()
        own[k] = value + core_in[k]
        y_copies.append(remote(own.at[k], y_in.at[k], y_send.at[k], y_recv.at[k], {'seq': across}))
        y_copies[-1].start()
    for k in range(4):
        own[4 + k] = partial(12 + k)
    z_copies = []
    for k in range(4):
        c_copies[4 + k].wait_recv()
        y_copies[k].wait_recv()
        own[4 + k] = own[4 + k] + core_in[4 + k] + y_in[k]
        step = (2 + k) % 4
        if step:
            z_copies.append(remote(own.at[4 + k], z_in.at[step - 1], z_send.at[step - 1], z_recv.at[step - 1],
                                   {'head': lax.rem(head + step, N_HEAD)}))
            z_copies[-1].start()
        else:
            mine = 4 + k
    for copy in z_copies:
        copy.wait_recv()
    here = column(core, side, head)
    y[:, pl.ds(here, width)] = (own[mine] + z_in[0] + z_in[1] + z_in[2]).astype(BF16)

    def spread(half, quarter, z, send, recv, device):
        at = y.at[:, pl.ds(column(half, quarter, z), width)]
        return remote(at, at, send, recv, device)

    sends = []

    def go(copy):
        copy.start()
        sends.append(copy)

    gz, gy, gc = {}, {}, {}
    for step in (2, 1, 3):
        gz[step] = spread(core, side, head, gz_send.at[step - 1], gz_recv.at[step - 1], {'head': lax.rem(head + step, N_HEAD)})
        go(gz[step])
    gy[0] = spread(core, side, head, gy_send.at[0], gy_recv.at[0], {'seq': across})
    gc[0] = spread(core, side, head, gc_send.at[0], gc_recv.at[0], {'seq': partner})
    go(gy[0])
    go(gc[0])
    for step in (1, 3, 2):
        source = lax.rem(head + N_HEAD - step, N_HEAD)
        gz[step].wait_recv()
        gy[step] = spread(core, side, source, gy_send.at[step], gy_recv.at[step], {'seq': across})
        gc[step] = spread(core, side, source, gc_send.at[step], gc_recv.at[step], {'seq': partner})
        go(gy[step])
        go(gc[step])
    for step in (0, 1, 3, 2):
        source = lax.rem(head + N_HEAD - step, N_HEAD)
        gy[step].wait_recv()
        gc[4 + step] = spread(core, 1 - side, source, gc_send.at[4 + step], gc_recv.at[4 + step], {'seq': partner})
        go(gc[4 + step])
    for step in range(8):
        gc[step].wait_recv()
    for copy in a_copies[:0] + c_copies + y_copies + z_copies + sends:
        copy.wait_send()


def output(mix, ml, w_out):
    rows, d_out = w_out.shape
    n_q = rows // LANES
    batch = mix.shape[0] // (N_SEQ * n_q)
    width = d_out // 16
    dma = pltpu.SemaphoreType.DMA
    return pl.pallas_call(
        output_kernel,
        out_shape=pltpu.VMEM((batch, d_out), BF16),
        in_specs=[VMEM, VMEM, HBM],
        out_specs=VMEM,
        scratch_shapes=[
            pltpu.VMEM((16, rows, width), BF16),
            pltpu.VMEM((3, n_q, batch, LANES), F32),
            pltpu.VMEM((3, 8, LANES), F32),
            pltpu.VMEM((batch, rows), BF16),
            pltpu.VMEM((8, batch, width), F32),
            pltpu.VMEM((8, batch, width), F32),
            pltpu.VMEM((8, batch, width), F32),
            pltpu.VMEM((4, batch, width), F32),
            pltpu.VMEM((3, batch, width), F32),
            dma((16,)),
            dma((3,)), dma((3,)), dma((3,)), dma((3,)),
            dma((8,)), dma((8,)), dma((4,)), dma((4,)), dma((3,)), dma((3,)),
            dma((3,)), dma((3,)), dma((4,)), dma((4,)), dma((8,)), dma((8,)),
        ],
        compiler_params=pltpu.CompilerParams(collective_id=1, has_side_effects=True, vmem_limit_bytes=24 * 2**20),
        name='output',
    )(mix.reshape(N_SEQ * n_q, batch, LANES), ml, in_hbm(w_out))


def solution(mesh):
    cache_spec = P('rep', 'seq', 'head', None)

    def local_step(tokens, w_query, w_key, w_value, w_out, k_cache, v_cache, positions):
        batch, shard_len, kv_local, head_dim = k_cache.shape
        flat = (batch, shard_len * kv_local, head_dim)
        qkv, k_held, v_held = project(tokens, w_query, w_key, w_value, k_cache.reshape(flat), v_cache.reshape(flat))
        k_new, v_new, mix, ml, _, _ = attend(positions, qkv, k_held, v_held, shard_len)
        y = output(mix, ml, w_out)
        return y, k_new.reshape(k_cache.shape), v_new.reshape(v_cache.shape)

    return jax.shard_map(
        local_step,
        mesh=mesh,
        in_specs=(P('rep', None), P(), P(), P(), P(('head', 'seq'), None), cache_spec, cache_spec, P('rep')),
        out_specs=(P('rep', None), cache_spec, cache_spec),
        check_vma=False,
    )
```

```python
import functools

import jax
import jax.numpy as jnp
from jax import lax
from jax.experimental import pallas as pl
from jax.experimental.pallas import tpu as pltpu
from jax.sharding import PartitionSpec as P

MESH = pl.DeviceIdType.MESH
HBM = pl.BlockSpec(memory_space=pltpu.HBM)
VMEM = pl.BlockSpec(memory_space=pltpu.VMEM)
SMEM = pl.BlockSpec(memory_space=pltpu.SMEM)
N_SEQ = 4
N_HEAD = 4
LANES = 128
F32 = jnp.float32
BF16 = jnp.bfloat16


def in_hbm(x):
    return pltpu.with_memory_space_constraint(x, pltpu.HBM)


def entry_barrier(axes):
    sem = pltpu.get_barrier_semaphore()
    count = 0
    for axis, size in axes:
        me = lax.axis_index(axis)
        for step in range(1, size):
            pl.semaphore_signal(sem, inc=1, device_id={axis: lax.rem(me + step, size)}, device_id_type=MESH)
            count += 1
    return lambda: pl.semaphore_wait(sem, count)


def project_kernel(n_chunk, ahead, tok_hbm, wq_hbm, wk_hbm, wv_hbm, k_hbm, v_hbm, out, kbuf, vbuf, tok, wq, wkv, acc, acc_kv, stage,
                   load_sem, cache_sem, send_sem, recv_sem):
    head, seq = lax.axis_index('head'), lax.axis_index('seq')
    q_cols, depth = wq.shape[2], wq.shape[1]
    n_q = q_cols // LANES
    batch = tok.shape[0]
    wait_peers = entry_barrier((('seq', N_SEQ),))

    q_at = pl.multiple_of((head * N_SEQ + seq) * q_cols, q_cols)
    kv_at = pl.multiple_of((head * 2 + lax.rem(seq, 2)) * LANES, LANES)

    def tok_copy(c):
        return pltpu.make_async_copy(tok_hbm.at[:, pl.ds(c * depth, depth)], tok.at[:, pl.ds(c * depth, depth)], load_sem.at[0, c])

    def q_copy(c):
        return pltpu.make_async_copy(wq_hbm.at[pl.ds(c * depth, depth), pl.ds(q_at, q_cols)], wq.at[c], load_sem.at[1, c])

    def kv_copy(src, c):
        return pltpu.make_async_copy(src.at[pl.ds(c * depth, depth), pl.ds(kv_at, LANES)], wkv.at[c], load_sem.at[2, c])

    def start(c):
        tok_copy(c).start()
        q_copy(c).start()

        @pl.when(seq < 2)
        def _():
            kv_copy(wk_hbm, c).start()

        @pl.when(seq >= 2)
        def _():
            kv_copy(wv_hbm, c).start()

    caches = []
    for g in range(8):
        span = pl.ds(g * (batch // 8), batch // 8)
        caches.append(pltpu.make_async_copy(k_hbm.at[span], kbuf.at[span], cache_sem.at[0, g]))
        caches.append(pltpu.make_async_copy(v_hbm.at[span], vbuf.at[span], cache_sem.at[1, g]))
    started = 0

    for c in range(ahead):
        start(c)
    for c in range(n_chunk):
        if c + ahead < n_chunk:
            start(c + ahead)
        else:
            for copy in caches[started:started + 4]:
                copy.start()
            started += 4
        tok_copy(c).wait()
        q_copy(c).wait()
        kv_copy(wk_hbm, c).wait()
        x = tok[:, c * depth:(c + 1) * depth]
        q_part = jnp.dot(x, wq[c], preferred_element_type=F32)
        kv_part = jnp.dot(x, wkv[c], preferred_element_type=F32)
        if c == 0:
            acc[...] = q_part
            acc_kv[...] = kv_part
        else:
            acc[...] += q_part
            acc_kv[...] += kv_part
    for i in range(n_q):
        stage[i] = acc[:, i * LANES:(i + 1) * LANES].astype(BF16)
    stage[n_q] = acc_kv[...].astype(BF16)

    wait_peers()
    copies = []
    for step in range(1, N_SEQ):
        copies.append(pltpu.make_async_remote_copy(
            src_ref=stage, dst_ref=out.at[seq], send_sem=send_sem.at[step - 1], recv_sem=recv_sem.at[step - 1],
            device_id={'seq': lax.rem(seq + step, N_SEQ)}, device_id_type=MESH))
        copies[-1].start()
    out[seq] = stage[...]
    for copy in copies:
        copy.wait()
    for copy in caches:
        copy.wait()


def project(tokens, w_query, w_key, w_value, k_cache, v_cache):
    batch, d_model = tokens.shape
    q_cols = w_query.shape[1] // (N_HEAD * N_SEQ)
    n_chunk = 8
    depth = d_model // n_chunk
    n_q = q_cols // LANES
    return pl.pallas_call(
        functools.partial(project_kernel, n_chunk, 4),
        out_shape=[pltpu.VMEM((N_SEQ, n_q + 1, batch, LANES), BF16), pltpu.VMEM(k_cache.shape, BF16), pltpu.VMEM(k_cache.shape, BF16)],
        in_specs=[HBM] * 6,
        out_specs=[VMEM] * 3,
        scratch_shapes=[
            pltpu.VMEM((batch, d_model), BF16),
            pltpu.VMEM((n_chunk, depth, q_cols), BF16),
            pltpu.VMEM((n_chunk, depth, LANES), BF16),
            pltpu.VMEM((batch, q_cols), F32),
            pltpu.VMEM((batch, LANES), F32),
            pltpu.VMEM((n_q + 1, batch, LANES), BF16),
            pltpu.SemaphoreType.DMA((3, n_chunk)),
            pltpu.SemaphoreType.DMA((2, 8)),
            pltpu.SemaphoreType.DMA((N_SEQ - 1,)),
            pltpu.SemaphoreType.DMA((N_SEQ - 1,)),
        ],
        compiler_params=pltpu.CompilerParams(collective_id=0, has_side_effects=True, vmem_limit_bytes=18 * 2**20),
        name='project',
    )(*map(in_hbm, (tokens, w_query, w_key, w_value, k_cache, v_cache)))


def attend_kernel(n_chunk, shard_len, pos_ref, qkv_ref, k_in, v_in, k_out, v_out, mix_out, ml_out, kbuf, vbuf,
                  qf, kvf, store_sem):
    batch, rows = kbuf.shape[0], kbuf.shape[1]
    n_q = qkv_ref.shape[1] - 1
    n_rows = N_SEQ * n_q
    per = batch // n_chunk
    start = lax.axis_index('seq') * shard_len

    def store(hbm, buf, which, c):
        return pltpu.make_async_copy(buf.at[pl.ds(c * per, per)], hbm.at[pl.ds(c * per, per)], store_sem.at[which, c])

    for s in range(N_SEQ):
        for i in range(n_q):
            at = (s * n_q + i) * batch
            qf[at:at + batch, :] = qkv_ref[s, i].astype(F32)
        kvf[s * batch:(s + 1) * batch, :] = qkv_ref[s, n_q].astype(F32)

    col = lax.broadcasted_iota(jnp.int32, (n_rows, rows), 1)
    row = lax.broadcasted_iota(jnp.int32, (n_rows, rows), 0)
    slot = jnp.where((col & 1) == row // (n_rows // 2), col >> 1, jnp.int32(1 << 30))
    win_row = lax.broadcasted_iota(jnp.int32, (16, LANES), 0)
    win_odd = (win_row & 1) == 1
    win_slot = win_row >> 1
    lane = lax.broadcasted_iota(jnp.int32, (n_rows, LANES), 1)

    def chunk(c, ml):
        for j in range(per):
            b = c * per + j
            pos = pos_ref[b] - start
            inside = jnp.logical_and(pos >= 0, pos < shard_len)
            slot_at = jnp.clip(pos, 0, shard_len - 1)
            base = pl.multiple_of((slot_at >> 3) * 16, 16)
            hit = win_slot == jnp.where(inside, slot_at & 7, -1)
            for buf, first in ((kbuf, 0), (vbuf, 2)):
                new = jnp.where(win_odd, kvf[pl.ds((first + 1) * batch + b, 1), :], kvf[pl.ds(first * batch + b, 1), :])
                old = buf[b, pl.ds(base, 16), :]
                buf[b, pl.ds(base, 16), :] = jnp.where(hit, new.astype(BF16), old)
        store(k_out, kbuf, 0, c).start()
        store(v_out, vbuf, 1, c).start()
        index = [c * per + j for j in range(per)]
        scores = []
        for b in index:
            q = qf[pl.ds(b, n_rows, stride=batch), :].astype(BF16)
            scores.append(lax.dot_general(q, kbuf[b], (((1,), (1,)), ((), ())), preferred_element_type=F32))
        weights = []
        for b, s in zip(index, scores):
            s = jnp.where(slot <= pos_ref[b] - start, s * LANES ** -0.5, -jnp.inf)
            m = jnp.max(s, axis=1, keepdims=True)
            w = jnp.exp(s - jnp.where(m == -jnp.inf, 0.0, m))
            l = jnp.sum(w, axis=1, keepdims=True)
            weights.append(w.astype(BF16))
            ml = jnp.where(lane == b, m, jnp.where(lane == batch + b, l, ml))
        for b, w in zip(index, weights):
            mix_out[pl.ds(b, n_rows, stride=batch), :] = jnp.dot(w, vbuf[b], preferred_element_type=F32)
        return ml

    ml = lax.fori_loop(0, n_chunk, chunk, jnp.zeros((n_rows, LANES), F32))
    ml_out[...] = jnp.zeros_like(ml_out)
    for s in range(N_SEQ):
        ml_out[s, 0:n_q, :] = ml[s * n_q:(s + 1) * n_q, :]
    for c in range(n_chunk):
        store(k_out, kbuf, 0, c).wait()
        store(v_out, vbuf, 1, c).wait()


def attend(positions, qkv, k_cache, v_cache, shard_len):
    batch, rows, _ = k_cache.shape
    n_rows = N_SEQ * (qkv.shape[1] - 1)
    n_chunk = 4
    cache = pltpu.HBM(k_cache.shape, BF16)
    held = pltpu.VMEM(k_cache.shape, BF16)
    return pl.pallas_call(
        functools.partial(attend_kernel, n_chunk, shard_len),
        out_shape=[cache, cache, pltpu.VMEM((n_rows * batch, LANES), F32), pltpu.VMEM((N_SEQ, 8, LANES), F32), held, held],
        in_specs=[SMEM, VMEM, VMEM, VMEM],
        out_specs=[HBM, HBM, VMEM, VMEM, VMEM, VMEM],
        input_output_aliases={2: 4, 3: 5},
        scratch_shapes=[
            pltpu.VMEM((n_rows * batch, LANES), F32),
            pltpu.VMEM((N_SEQ * batch, LANES), F32),
            pltpu.SemaphoreType.DMA((2, n_chunk)),
        ],
        compiler_params=pltpu.CompilerParams(vmem_limit_bytes=6 * 2**20),
        name='attend',
    )(positions, qkv, k_cache, v_cache)


def output_kernel(mix, ml, wo_hbm, y, wo, mix_in, ml_in, attn, give, own, core_in, y_in, z_in,
                  wo_sem, a_send, a_recv, m_send, m_recv, c_send, c_recv, y_send, y_recv, z_send, z_recv,
                  gz_send, gz_recv, gy_send, gy_recv, gc_send, gc_recv):
    head, seq = lax.axis_index('head'), lax.axis_index('seq')
    side, core = seq // 2, lax.rem(seq, 2)
    partner = side * 2 + (1 - core)
    across = (1 - side) * 2 + core
    n_q, batch = mix_in.shape[1], mix_in.shape[2]
    width = own.shape[2]
    wait_peers = entry_barrier((('seq', N_SEQ), ('head', N_HEAD)))

    def place(k):
        half = (1 - core) if k < 8 else core
        quarter = (1 - side) if (k % 8) < 4 else side
        z = lax.rem(head + 2 + k % 4, N_HEAD)
        return half, quarter, z

    def column(half, quarter, z):
        return pl.multiple_of(((half * 2 + quarter) * N_HEAD + z) * width, width)

    def wo_copy(k):
        return pltpu.make_async_copy(wo_hbm.at[:, pl.ds(column(*place(k)), width)], wo.at[k], wo_sem.at[k])

    for k in range(16):
        wo_copy(k).start()

    def remote(src, dst, send, recv, device):
        return pltpu.make_async_remote_copy(src_ref=src, dst_ref=dst, send_sem=send, recv_sem=recv, device_id=device, device_id_type=MESH)

    wait_peers()
    a_copies = []
    for step in range(1, N_SEQ):
        to = lax.rem(seq + step, N_SEQ)
        a_copies.append(remote(ml.at[to], ml_in.at[step - 1], m_send.at[step - 1], m_recv.at[step - 1], {'seq': to}))
        a_copies.append(remote(mix.at[pl.ds(to * n_q, n_q)], mix_in.at[step - 1], a_send.at[step - 1], a_recv.at[step - 1], {'seq': to}))
    for copy in a_copies:
        copy.start()
    for copy in a_copies:
        copy.wait()

    parts = [ml[seq]] + [ml_in[i] for i in range(N_SEQ - 1)]
    top = functools.reduce(jnp.maximum, parts)
    scales = [jnp.exp(p - top) for p in parts]
    total = functools.reduce(jnp.add, [pltpu.roll(p, LANES - batch, 1) * e for p, e in zip(parts, scales)])
    scales = [e / total for e in scales]
    table = jnp.concatenate(scales + [jnp.zeros((LANES - 8 * N_SEQ, LANES), F32)], axis=0).T
    for i in range(n_q):
        acc = mix[seq * n_q + i] * table[0:batch, i:i + 1]
        for s in range(1, N_SEQ):
            acc += mix_in[s - 1, i] * table[0:batch, s * 8 + i:s * 8 + i + 1]
        attn[:, i * LANES:(i + 1) * LANES] = acc.astype(BF16)

    def partial(k):
        wo_copy(k).wait()
        return jnp.dot(attn[...], wo[k], preferred_element_type=F32)

    c_copies = []
    for k in range(8):
        give[k] = partial(k)
        c_copies.append(remote(give.at[k], core_in.at[k], c_send.at[k], c_recv.at[k], {'seq': partner}))
        c_copies[-1].start()
    y_copies = []
    for k in range(4):
        value = partial(8 + k)
        c_copies[k].wait_recv()
        own[k] = value + core_in[k]
        y_copies.append(remote(own.at[k], y_in.at[k], y_send.at[k], y_recv.at[k], {'seq': across}))
        y_copies[-1].start()
    for k in range(4):
        own[4 + k] = partial(12 + k)
    z_copies = []
    for k in range(4):
        c_copies[4 + k].wait_recv()
        y_copies[k].wait_recv()
        own[4 + k] = own[4 + k] + core_in[4 + k] + y_in[k]
        step = (2 + k) % 4
        if step:
            z_copies.append(remote(own.at[4 + k], z_in.at[step - 1], z_send.at[step - 1], z_recv.at[step - 1],
                                   {'head': lax.rem(head + step, N_HEAD)}))
            z_copies[-1].start()
        else:
            mine = 4 + k
    for copy in z_copies:
        copy.wait_recv()
    here = column(core, side, head)
    y[:, pl.ds(here, width)] = (own[mine] + z_in[0] + z_in[1] + z_in[2]).astype(BF16)

    def spread(half, quarter, z, send, recv, device):
        at = y.at[:, pl.ds(column(half, quarter, z), width)]
        return remote(at, at, send, recv, device)

    sends = []

    def go(copy):
        copy.start()
        sends.append(copy)

    gz, gy, gc = {}, {}, {}
    for step in (2, 1, 3):
        gz[step] = spread(core, side, head, gz_send.at[step - 1], gz_recv.at[step - 1], {'head': lax.rem(head + step, N_HEAD)})
        go(gz[step])
    gy[0] = spread(core, side, head, gy_send.at[0], gy_recv.at[0], {'seq': across})
    gc[0] = spread(core, side, head, gc_send.at[0], gc_recv.at[0], {'seq': partner})
    go(gy[0])
    go(gc[0])
    for step in (1, 3, 2):
        source = lax.rem(head + N_HEAD - step, N_HEAD)
        gz[step].wait_recv()
        gy[step] = spread(core, side, source, gy_send.at[step], gy_recv.at[step], {'seq': across})
        gc[step] = spread(core, side, source, gc_send.at[step], gc_recv.at[step], {'seq': partner})
        go(gy[step])
        go(gc[step])
    for step in (0, 1, 3, 2):
        source = lax.rem(head + N_HEAD - step, N_HEAD)
        gy[step].wait_recv()
        gc[4 + step] = spread(core, 1 - side, source, gc_send.at[4 + step], gc_recv.at[4 + step], {'seq': partner})
        go(gc[4 + step])
    for step in range(8):
        gc[step].wait_recv()
    for copy in a_copies[:0] + c_copies + y_copies + z_copies + sends:
        copy.wait_send()


def output(mix, ml, w_out):
    rows, d_out = w_out.shape
    n_q = rows // LANES
    batch = mix.shape[0] // (N_SEQ * n_q)
    width = d_out // 16
    dma = pltpu.SemaphoreType.DMA
    return pl.pallas_call(
        output_kernel,
        out_shape=pltpu.VMEM((batch, d_out), BF16),
        in_specs=[VMEM, VMEM, HBM],
        out_specs=VMEM,
        scratch_shapes=[
            pltpu.VMEM((16, rows, width), BF16),
            pltpu.VMEM((3, n_q, batch, LANES), F32),
            pltpu.VMEM((3, 8, LANES), F32),
            pltpu.VMEM((batch, rows), BF16),
            pltpu.VMEM((8, batch, width), F32),
            pltpu.VMEM((8, batch, width), F32),
            pltpu.VMEM((8, batch, width), F32),
            pltpu.VMEM((4, batch, width), F32),
            pltpu.VMEM((3, batch, width), F32),
            dma((16,)),
            dma((3,)), dma((3,)), dma((3,)), dma((3,)),
            dma((8,)), dma((8,)), dma((4,)), dma((4,)), dma((3,)), dma((3,)),
            dma((3,)), dma((3,)), dma((4,)), dma((4,)), dma((8,)), dma((8,)),
        ],
        compiler_params=pltpu.CompilerParams(collective_id=1, has_side_effects=True, vmem_limit_bytes=24 * 2**20),
        name='output',
    )(mix.reshape(N_SEQ * n_q, batch, LANES), ml, in_hbm(w_out))


def solution(mesh):
    cache_spec = P('rep', 'seq', 'head', None)

    def local_step(tokens, w_query, w_key, w_value, w_out, k_cache, v_cache, positions):
        batch, shard_len, kv_local, head_dim = k_cache.shape
        flat = (batch, shard_len * kv_local, head_dim)
        qkv, k_held, v_held = project(tokens, w_query, w_key, w_value, k_cache.reshape(flat), v_cache.reshape(flat))
        k_new, v_new, mix, ml, _, _ = attend(positions, qkv, k_held, v_held, shard_len)
        y = output(mix, ml, w_out)
        return y, k_new.reshape(k_cache.shape), v_new.reshape(v_cache.shape)

    return jax.shard_map(
        local_step,
        mesh=mesh,
        in_specs=(P('rep', None), P(), P(), P(), P(('head', 'seq'), None), cache_spec, cache_spec, P('rep')),
        out_specs=(P('rep', None), cache_spec, cache_spec),
        check_vma=False,
    )
```

```python
import functools

import jax
import jax.numpy as jnp
from jax import lax
from jax.experimental import pallas as pl
from jax.experimental.pallas import tpu as pltpu
from jax.sharding import PartitionSpec as P

MESH = pl.DeviceIdType.MESH
HBM = pl.BlockSpec(memory_space=pltpu.HBM)
VMEM = pl.BlockSpec(memory_space=pltpu.VMEM)
SMEM = pl.BlockSpec(memory_space=pltpu.SMEM)
N_SEQ = 4
N_HEAD = 4
LANES = 128
F32 = jnp.float32
BF16 = jnp.bfloat16


def in_hbm(x):
    return pltpu.with_memory_space_constraint(x, pltpu.HBM)


def entry_barrier(axes):
    sem = pltpu.get_barrier_semaphore()
    count = 0
    for axis, size in axes:
        me = lax.axis_index(axis)
        for step in range(1, size):
            pl.semaphore_signal(sem, inc=1, device_id={axis: lax.rem(me + step, size)}, device_id_type=MESH)
            count += 1
    return lambda: pl.semaphore_wait(sem, count)


def project_kernel(n_chunk, ahead, tok_hbm, wq_hbm, wk_hbm, wv_hbm, k_hbm, v_hbm, out, kbuf, vbuf, tok, w_first, w_second,
                   acc_first, acc_second, stage, load_sem, cache_sem, send_sem, recv_sem):
    head, seq = lax.axis_index('head'), lax.axis_index('seq')
    depth = w_first.shape[1]
    batch = tok.shape[0]
    wait_peers = entry_barrier((('seq', N_SEQ),))

    second = w_second.shape[2]
    first = w_first.shape[2] - LANES
    q_at = (head * N_SEQ + seq) * (first + second)
    kv_at = pl.multiple_of((head * 2 + lax.rem(seq, 2)) * LANES, LANES)

    def tok_copy(c):
        return pltpu.make_async_copy(tok_hbm.at[:, pl.ds(c * depth, depth)], tok.at[:, pl.ds(c * depth, depth)], load_sem.at[0, c])

    def kv_copy(src, c):
        return pltpu.make_async_copy(src.at[pl.ds(c * depth, depth), pl.ds(kv_at, LANES)], w_first.at[c, :, pl.ds(0, LANES)],
                                     load_sem.at[1, c])

    def q_copy(r, c):
        rows = pl.ds(c * depth, depth)
        if r == 0:
            at = pl.multiple_of(q_at, LANES)
            return pltpu.make_async_copy(wq_hbm.at[rows, pl.ds(at, first)], w_first.at[c, :, pl.ds(LANES, first)], load_sem.at[2, c])
        at = pl.multiple_of(q_at + first, LANES)
        return pltpu.make_async_copy(wq_hbm.at[rows, pl.ds(at, second)], w_second.at[c], load_sem.at[3, c])

    def start(r, c):
        q_copy(r, c).start()
        if r == 0:
            tok_copy(c).start()

            @pl.when(seq < 2)
            def _():
                kv_copy(wk_hbm, c).start()

            @pl.when(seq >= 2)
            def _():
                kv_copy(wv_hbm, c).start()

    caches = []
    for g in range(8):
        span = pl.ds(g * (batch // 8), batch // 8)
        caches.append(pltpu.make_async_copy(k_hbm.at[span], kbuf.at[span], cache_sem.at[0, g]))
        caches.append(pltpu.make_async_copy(v_hbm.at[span], vbuf.at[span], cache_sem.at[1, g]))
    share = len(caches) // ahead
    held = 0

    turns = [(r, c) for r in range(2) for c in range(n_chunk)]
    copies = []
    for r, c in turns[:ahead]:
        start(r, c)
    for n, (r, c) in enumerate(turns):
        if n + ahead < len(turns):
            start(*turns[n + ahead])
        else:
            for copy in caches[held:held + share]:
                copy.start()
            held += share
        q_copy(r, c).wait()
        if r == 0:
            tok_copy(c).wait()
            kv_copy(wk_hbm, c).wait()
        acc, w = ((acc_first, w_first), (acc_second, w_second))[r]
        part = jnp.dot(tok[:, c * depth:(c + 1) * depth], w[c], preferred_element_type=F32)
        if c == 0:
            acc[...] = part
        else:
            acc[...] += part
        if c == n_chunk - 1:
            at, count = (0, acc.shape[1] // LANES) if r == 0 else (w_first.shape[2] // LANES, acc.shape[1] // LANES)
            for i in range(count):
                stage[at + i] = acc[:, i * LANES:(i + 1) * LANES].astype(BF16)
            if r == 0:
                wait_peers()
            for step in (2, 1, 3):
                copies.append(pltpu.make_async_remote_copy(
                    src_ref=stage.at[pl.ds(at, count)], dst_ref=out.at[seq, pl.ds(at, count)],
                    send_sem=send_sem.at[r, step - 1], recv_sem=recv_sem.at[r, step - 1],
                    device_id={'seq': lax.rem(seq + step, N_SEQ)}, device_id_type=MESH))
                copies[-1].start()
            out[seq, at:at + count] = stage[at:at + count]
    for copy in copies:
        copy.wait()
    for copy in caches:
        copy.wait()


def project(tokens, w_query, w_key, w_value, k_cache, v_cache):
    batch, d_model = tokens.shape
    q_cols = w_query.shape[1] // (N_HEAD * N_SEQ)
    n_chunk = 8
    depth = d_model // n_chunk
    n_q = q_cols // LANES
    first = LANES + q_cols // 2
    second = q_cols - q_cols // 2
    return pl.pallas_call(
        functools.partial(project_kernel, n_chunk, 8),
        out_shape=[pltpu.VMEM((N_SEQ, n_q + 1, batch, LANES), BF16), pltpu.VMEM(k_cache.shape, BF16), pltpu.VMEM(k_cache.shape, BF16)],
        in_specs=[HBM] * 6,
        out_specs=[VMEM] * 3,
        scratch_shapes=[
            pltpu.VMEM((batch, d_model), BF16),
            pltpu.VMEM((n_chunk, depth, first), BF16),
            pltpu.VMEM((n_chunk, depth, second), BF16),
            pltpu.VMEM((batch, first), F32),
            pltpu.VMEM((batch, second), F32),
            pltpu.VMEM((n_q + 1, batch, LANES), BF16),
            pltpu.SemaphoreType.DMA((4, n_chunk)),
            pltpu.SemaphoreType.DMA((2, 8)),
            pltpu.SemaphoreType.DMA((2, N_SEQ - 1)),
            pltpu.SemaphoreType.DMA((2, N_SEQ - 1)),
        ],
        compiler_params=pltpu.CompilerParams(collective_id=0, has_side_effects=True, vmem_limit_bytes=18 * 2**20),
        name='project',
    )(*map(in_hbm, (tokens, w_query, w_key, w_value, k_cache, v_cache)))


def attend_kernel(n_chunk, shard_len, pos_ref, qkv_ref, k_in, v_in, k_out, v_out, mix_out, ml_out, kbuf, vbuf,
                  qf, kvf, store_sem):
    batch, rows = kbuf.shape[0], kbuf.shape[1]
    n_q = qkv_ref.shape[1] - 1
    n_rows = N_SEQ * n_q
    per = batch // n_chunk
    start = lax.axis_index('seq') * shard_len

    def store(hbm, buf, which, c):
        return pltpu.make_async_copy(buf.at[pl.ds(c * per, per)], hbm.at[pl.ds(c * per, per)], store_sem.at[which, c])

    for s in range(N_SEQ):
        for i in range(n_q):
            at = (s * n_q + i) * batch
            qf[at:at + batch, :] = qkv_ref[s, 1 + i].astype(F32)
        kvf[s * batch:(s + 1) * batch, :] = qkv_ref[s, 0].astype(F32)

    col = lax.broadcasted_iota(jnp.int32, (n_rows, rows), 1)
    row = lax.broadcasted_iota(jnp.int32, (n_rows, rows), 0)
    slot = jnp.where((col & 1) == row // (n_rows // 2), col >> 1, jnp.int32(1 << 30))
    win_row = lax.broadcasted_iota(jnp.int32, (16, LANES), 0)
    win_odd = (win_row & 1) == 1
    win_slot = win_row >> 1
    lane = lax.broadcasted_iota(jnp.int32, (n_rows, LANES), 1)

    def chunk(c, ml):
        for j in range(per):
            b = c * per + j
            pos = pos_ref[b] - start
            inside = jnp.logical_and(pos >= 0, pos < shard_len)
            slot_at = jnp.clip(pos, 0, shard_len - 1)
            base = pl.multiple_of((slot_at >> 3) * 16, 16)
            hit = win_slot == jnp.where(inside, slot_at & 7, -1)
            for buf, first in ((kbuf, 0), (vbuf, 2)):
                new = jnp.where(win_odd, kvf[pl.ds((first + 1) * batch + b, 1), :], kvf[pl.ds(first * batch + b, 1), :])
                old = buf[b, pl.ds(base, 16), :]
                buf[b, pl.ds(base, 16), :] = jnp.where(hit, new.astype(BF16), old)
        store(k_out, kbuf, 0, c).start()
        store(v_out, vbuf, 1, c).start()
        index = [c * per + j for j in range(per)]
        scores = []
        for b in index:
            q = qf[pl.ds(b, n_rows, stride=batch), :].astype(BF16)
            scores.append(lax.dot_general(q, kbuf[b], (((1,), (1,)), ((), ())), preferred_element_type=F32))
        weights = []
        for b, s in zip(index, scores):
            s = jnp.where(slot <= pos_ref[b] - start, s * LANES ** -0.5, -jnp.inf)
            m = jnp.max(s, axis=1, keepdims=True)
            w = jnp.exp(s - jnp.where(m == -jnp.inf, 0.0, m))
            l = jnp.sum(w, axis=1, keepdims=True)
            weights.append(w.astype(BF16))
            ml = jnp.where(lane == b, m, jnp.where(lane == batch + b, l, ml))
        for b, w in zip(index, weights):
            mix_out[pl.ds(b, n_rows, stride=batch), :] = jnp.dot(w, vbuf[b], preferred_element_type=F32)
        return ml

    ml = lax.fori_loop(0, n_chunk, chunk, jnp.zeros((n_rows, LANES), F32))
    ml_out[...] = jnp.zeros_like(ml_out)
    for s in range(N_SEQ):
        ml_out[s, 0:n_q, :] = ml[s * n_q:(s + 1) * n_q, :]
    for c in range(n_chunk):
        store(k_out, kbuf, 0, c).wait()
        store(v_out, vbuf, 1, c).wait()


def attend(positions, qkv, k_cache, v_cache, shard_len):
    batch, rows, _ = k_cache.shape
    n_rows = N_SEQ * (qkv.shape[1] - 1)
    n_chunk = 4
    cache = pltpu.HBM(k_cache.shape, BF16)
    held = pltpu.VMEM(k_cache.shape, BF16)
    return pl.pallas_call(
        functools.partial(attend_kernel, n_chunk, shard_len),
        out_shape=[cache, cache, pltpu.VMEM((n_rows * batch, LANES), F32), pltpu.VMEM((N_SEQ, 8, LANES), F32), held, held],
        in_specs=[SMEM, VMEM, VMEM, VMEM],
        out_specs=[HBM, HBM, VMEM, VMEM, VMEM, VMEM],
        input_output_aliases={2: 4, 3: 5},
        scratch_shapes=[
            pltpu.VMEM((n_rows * batch, LANES), F32),
            pltpu.VMEM((N_SEQ * batch, LANES), F32),
            pltpu.SemaphoreType.DMA((2, n_chunk)),
        ],
        compiler_params=pltpu.CompilerParams(vmem_limit_bytes=6 * 2**20),
        name='attend',
    )(positions, qkv, k_cache, v_cache)


def lane_table(rows):
    fill = jnp.zeros((LANES - 8 * len(rows), LANES), F32)
    return jnp.concatenate(list(rows) + [fill], axis=0).T


def merge(parts, batch):
    top = functools.reduce(jnp.maximum, parts)
    safe = jnp.where(top == -jnp.inf, 0.0, top)
    factors = [jnp.exp(p - safe) for p in parts]
    total = functools.reduce(jnp.add, [pltpu.roll(p, LANES - batch, 1) * e for p, e in zip(parts, factors)])
    return top, total, factors


def output_kernel(n_pass, mix, ml, wo_hbm, y, wo, pair_in, far_in, pair_ml, far_ml, far_give, far_give_ml, attn, give, own, core_in, y_in, z_in,
                  wo_sem, p_send, p_recv, f_send, f_recv, c_send, c_recv, y_send, y_recv, z_send, z_recv,
                  gz_send, gz_recv, gy_send, gy_recv, gc_send, gc_recv):
    head, seq = lax.axis_index('head'), lax.axis_index('seq')
    side, core = seq // 2, lax.rem(seq, 2)
    partner = side * 2 + (1 - core)
    across = (1 - side) * 2 + core
    diagonal = (1 - side) * 2 + (1 - core)
    n_q, batch = pair_in.shape[1], pair_in.shape[2]
    narrow = z_in.shape[3]
    wait_peers = entry_barrier((('seq', N_SEQ), ('head', N_HEAD)))

    def column(half, quarter, z, p):
        return pl.multiple_of((((half * 2 + quarter) * N_HEAD + z) * n_pass + p) * narrow, narrow)

    def unit(mine, near, p):
        return ((1 if mine else 0) * 2 + (1 if near else 0)) * n_pass + p

    def wo_copy(mine, near, p, j):
        at = column(core if mine else 1 - core, side if near else 1 - side, lax.rem(head + j, N_HEAD), p)
        u = unit(mine, near, p)
        return pltpu.make_async_copy(wo_hbm.at[:, pl.ds(at, narrow)], wo.at[u, :, pl.ds(j * narrow, narrow)], wo_sem.at[u, j])

    order = [(mine, near, p) for near in (False, True) for mine in (False, True) for p in range(n_pass)]
    for mine, near, p in order:
        for j in range(N_HEAD):
            wo_copy(mine, near, p, j).start()

    def remote(src, dst, send, recv, device):
        copy = pltpu.make_async_remote_copy(src_ref=src, dst_ref=dst, send_sem=send, recv_sem=recv, device_id=device, device_id_type=MESH)
        copy.start()
        return copy

    wait_peers()
    pair = []
    for n, to in enumerate((diagonal, partner)):
        pair.append(remote(ml.at[to], pair_ml.at[n], p_send.at[0, n], p_recv.at[0, n], {'seq': partner}))
        pair.append(remote(mix.at[pl.ds(to * n_q, n_q)], pair_in.at[n], p_send.at[1, n], p_recv.at[1, n], {'seq': partner}))
    pair[0].wait_recv()
    pair[1].wait_recv()
    top, total, factors = merge([ml[across], pair_ml[0]], batch)
    lane = lax.broadcasted_iota(jnp.int32, (8, LANES), 1)
    far_give_ml[...] = jnp.where(lane < batch, top, pltpu.roll(total, batch, 1))
    table = lane_table(factors)
    for i in range(n_q):
        far_give[i] = mix[across * n_q + i] * table[0:batch, i:i + 1] + pair_in[0, i] * table[0:batch, 8 + i:9 + i]
    far = [remote(far_give_ml, far_ml, f_send.at[0], f_recv.at[0], {'seq': across}),
           remote(far_give, far_in, f_send.at[1], f_recv.at[1], {'seq': across})]
    pair[2].wait_recv()
    pair[3].wait_recv()
    for copy in far:
        copy.wait_recv()
    _, total, factors = merge([ml[seq], pair_ml[1], far_ml[...]], batch)
    table = lane_table([e / total for e in factors])
    for i in range(n_q):
        value = mix[seq * n_q + i] * table[0:batch, i:i + 1]
        value += pair_in[1, i] * table[0:batch, 8 + i:9 + i]
        value += far_in[i] * table[0:batch, 16 + i:17 + i]
        attn[:, i * LANES:(i + 1) * LANES] = value.astype(BF16)
    sends = pair + far

    for mine, near, p in order:
        for j in range(N_HEAD):
            wo_copy(mine, near, p, j).wait()

    def partial(mine, near, p):
        return jnp.dot(attn[...], wo[unit(mine, near, p)], preferred_element_type=F32)

    def hand(near, p):
        u = unit(False, near, p)
        give[u] = partial(False, near, p)
        c_copies[near, p] = remote(give.at[u], core_in.at[u], c_send.at[u], c_recv.at[u], {'seq': partner})

    def keep(near, p):
        u = unit(False, near, p)
        value = partial(True, near, p)
        c_copies[near, p].wait_recv()
        own[u] = value + core_in[u]

    c_copies, y_copies, z_copies = {}, {}, {}
    for p in range(n_pass):
        hand(False, p)
    for p in range(n_pass):
        keep(False, p)
        y_copies[p] = remote(own.at[unit(False, False, p)], y_in.at[p], y_send.at[p], y_recv.at[p], {'seq': across})
    for p in range(n_pass):
        hand(True, p)
    for p in range(n_pass):
        keep(True, p)

    def along(p):
        u = unit(False, True, p)
        y_copies[p].wait_recv()
        own[u] = own[u] + y_in[p]
        for step in (2, 1, 3):
            z_copies[p, step] = remote(own.at[u, :, pl.ds(step * narrow, narrow)], z_in.at[p, step - 1], z_send.at[p, step - 1],
                                       z_recv.at[p, step - 1], {'head': lax.rem(head + step, N_HEAD)})

    def spread(half, quarter, z, p, send, recv, device):
        at = y.at[:, pl.ds(column(half, quarter, z, p), narrow)]
        return remote(at, at, send, recv, device)

    gz, gy, gc = {}, {}, {}

    def fan(z, p, step):
        gy[p, step] = spread(core, side, z, p, gy_send.at[p, step], gy_recv.at[p, step], {'seq': across})
        gc[p, step] = spread(core, side, z, p, gc_send.at[p, step], gc_recv.at[p, step], {'seq': partner})

    def finish(p):
        for step in (1, 3, 2):
            z_copies[p, step].wait_recv()
        value = own[unit(False, True, p), :, 0:narrow] + z_in[p, 0] + z_in[p, 1] + z_in[p, 2]
        y[:, pl.ds(column(core, side, head, p), narrow)] = value.astype(BF16)
        for step in (2, 1, 3):
            gz[p, step] = spread(core, side, head, p, gz_send.at[p, step - 1], gz_recv.at[p, step - 1], {'head': lax.rem(head + step, N_HEAD)})
        fan(head, p, 0)

    def over(p):
        for step in (1, 3, 2):
            gz[p, step].wait_recv()
            fan(lax.rem(head + N_HEAD - step, N_HEAD), p, step)

    def to_partner(p):
        for step in (0, 1, 3, 2):
            gy[p, step].wait_recv()
            z = lax.rem(head + N_HEAD - step, N_HEAD)
            gc[p, 4 + step] = spread(core, 1 - side, z, p, gc_send.at[p, 4 + step], gc_recv.at[p, 4 + step], {'seq': partner})

    stages = [(3 * p + at, n, p) for n, at in enumerate((0, 4.6, 9.3, 11.4)) for p in range(n_pass)]
    for _, n, p in sorted(stages):
        (along, finish, over, to_partner)[n](p)
    for copy in gc.values():
        copy.wait_recv()
    for group in (sends, *(g.values() for g in (c_copies, y_copies, z_copies, gz, gy, gc))):
        for copy in group:
            copy.wait_send()


def output(mix, ml, w_out):
    rows, d_out = w_out.shape
    n_q = rows // LANES
    batch = mix.shape[0] // (N_SEQ * n_q)
    n_pass = 4
    width = d_out // 16
    narrow = width // n_pass
    dma = pltpu.SemaphoreType.DMA
    block = pltpu.VMEM((n_q, batch, LANES), F32)
    return pl.pallas_call(
        functools.partial(output_kernel, n_pass),
        out_shape=pltpu.VMEM((batch, d_out), BF16),
        in_specs=[VMEM, VMEM, HBM],
        out_specs=VMEM,
        scratch_shapes=[
            pltpu.VMEM((4 * n_pass, rows, N_HEAD * narrow), BF16),
            pltpu.VMEM((2, n_q, batch, LANES), F32),
            block,
            pltpu.VMEM((2, 8, LANES), F32),
            pltpu.VMEM((8, LANES), F32),
            block,
            pltpu.VMEM((8, LANES), F32),
            pltpu.VMEM((batch, rows), BF16),
            pltpu.VMEM((2 * n_pass, batch, width), F32),
            pltpu.VMEM((2 * n_pass, batch, width), F32),
            pltpu.VMEM((2 * n_pass, batch, width), F32),
            pltpu.VMEM((n_pass, batch, width), F32),
            pltpu.VMEM((n_pass, 3, batch, narrow), F32),
            dma((4 * n_pass, N_HEAD)),
            dma((2, 2)), dma((2, 2)), dma((2,)), dma((2,)),
            dma((2 * n_pass,)), dma((2 * n_pass,)), dma((n_pass,)), dma((n_pass,)), dma((n_pass, 3)), dma((n_pass, 3)),
            dma((n_pass, 3)), dma((n_pass, 3)), dma((n_pass, 4)), dma((n_pass, 4)), dma((n_pass, 8)), dma((n_pass, 8)),
        ],
        compiler_params=pltpu.CompilerParams(collective_id=1, has_side_effects=True, vmem_limit_bytes=24 * 2**20),
        name='output',
    )(mix.reshape(N_SEQ * n_q, batch, LANES), ml, in_hbm(w_out))


def solution(mesh):
    cache_spec = P('rep', 'seq', 'head', None)

    def local_step(tokens, w_query, w_key, w_value, w_out, k_cache, v_cache, positions):
        batch, shard_len, kv_local, head_dim = k_cache.shape
        flat = (batch, shard_len * kv_local, head_dim)
        qkv, k_held, v_held = project(tokens, w_query, w_key, w_value, k_cache.reshape(flat), v_cache.reshape(flat))
        k_new, v_new, mix, ml, _, _ = attend(positions, qkv, k_held, v_held, shard_len)
        y = output(mix, ml, w_out)
        return y, k_new.reshape(k_cache.shape), v_new.reshape(v_cache.shape)

    return jax.shard_map(
        local_step,
        mesh=mesh,
        in_specs=(P('rep', None), P(), P(), P(), P(('head', 'seq'), None), cache_spec, cache_spec, P('rep')),
        out_specs=(P('rep', None), cache_spec, cache_spec),
        check_vma=False,
    )
```

```python
import functools

import jax
import jax.numpy as jnp
from jax import lax
from jax.experimental import pallas as pl
from jax.experimental.pallas import tpu as pltpu
from jax.sharding import PartitionSpec as P

MESH = pl.DeviceIdType.MESH
HBM = pl.BlockSpec(memory_space=pltpu.HBM)
VMEM = pl.BlockSpec(memory_space=pltpu.VMEM)
SMEM = pl.BlockSpec(memory_space=pltpu.SMEM)
N_SEQ = 4
N_HEAD = 4
LANES = 128
F32 = jnp.float32
BF16 = jnp.bfloat16


def in_hbm(x):
    return pltpu.with_memory_space_constraint(x, pltpu.HBM)


def entry_barrier(axes):
    sem = pltpu.get_barrier_semaphore()
    count = 0
    for axis, size in axes:
        me = lax.axis_index(axis)
        for step in range(1, size):
            pl.semaphore_signal(sem, inc=1, device_id={axis: lax.rem(me + step, size)}, device_id_type=MESH)
            count += 1
    return lambda: pl.semaphore_wait(sem, count)


def project_kernel(n_chunk, ahead, tok_hbm, wq_hbm, wk_hbm, wv_hbm, k_hbm, v_hbm, out, kbuf, vbuf, tok, w_first, w_second,
                   acc_first, acc_second, stage, load_sem, cache_sem, send_sem, recv_sem):
    head, seq = lax.axis_index('head'), lax.axis_index('seq')
    depth = w_first.shape[1]
    batch = tok.shape[0]
    wait_peers = entry_barrier((('seq', N_SEQ),))

    second = w_second.shape[2]
    first = w_first.shape[2] - LANES
    q_at = (head * N_SEQ + seq) * (first + second)
    kv_at = pl.multiple_of((head * 2 + lax.rem(seq, 2)) * LANES, LANES)

    def tok_copy(c):
        return pltpu.make_async_copy(tok_hbm.at[:, pl.ds(c * depth, depth)], tok.at[:, pl.ds(c * depth, depth)], load_sem.at[0, c])

    def kv_copy(src, c):
        return pltpu.make_async_copy(src.at[pl.ds(c * depth, depth), pl.ds(kv_at, LANES)], w_first.at[c, :, pl.ds(0, LANES)],
                                     load_sem.at[1, c])

    def q_copy(r, c):
        rows = pl.ds(c * depth, depth)
        if r == 0:
            at = pl.multiple_of(q_at, LANES)
            return pltpu.make_async_copy(wq_hbm.at[rows, pl.ds(at, first)], w_first.at[c, :, pl.ds(LANES, first)], load_sem.at[2, c])
        at = pl.multiple_of(q_at + first, LANES)
        return pltpu.make_async_copy(wq_hbm.at[rows, pl.ds(at, second)], w_second.at[c], load_sem.at[3, c])

    def start(r, c):
        q_copy(r, c).start()
        if r == 0:
            tok_copy(c).start()

            @pl.when(seq < 2)
            def _():
                kv_copy(wk_hbm, c).start()

            @pl.when(seq >= 2)
            def _():
                kv_copy(wv_hbm, c).start()

    caches = []
    for g in range(8):
        span = pl.ds(g * (batch // 8), batch // 8)
        caches.append(pltpu.make_async_copy(k_hbm.at[span], kbuf.at[span], cache_sem.at[0, g]))
        caches.append(pltpu.make_async_copy(v_hbm.at[span], vbuf.at[span], cache_sem.at[1, g]))
    share = len(caches) // ahead
    held = 0

    turns = [(r, c) for r in range(2) for c in range(n_chunk)]
    copies = []
    for r, c in turns[:ahead]:
        start(r, c)
    for n, (r, c) in enumerate(turns):
        if n + ahead < len(turns):
            start(*turns[n + ahead])
        else:
            for copy in caches[held:held + share]:
                copy.start()
            held += share
        q_copy(r, c).wait()
        if r == 0:
            tok_copy(c).wait()
            kv_copy(wk_hbm, c).wait()
        acc, w = ((acc_first, w_first), (acc_second, w_second))[r]
        part = jnp.dot(tok[:, c * depth:(c + 1) * depth], w[c], preferred_element_type=F32)
        if c == 0:
            acc[...] = part
        else:
            acc[...] += part
        if c == n_chunk - 1:
            at, count = (0, acc.shape[1] // LANES) if r == 0 else (w_first.shape[2] // LANES, acc.shape[1] // LANES)
            for i in range(count):
                stage[at + i] = acc[:, i * LANES:(i + 1) * LANES].astype(BF16)
            if r == 0:
                wait_peers()
            for step in (2, 1, 3):
                copies.append(pltpu.make_async_remote_copy(
                    src_ref=stage.at[pl.ds(at, count)], dst_ref=out.at[seq, pl.ds(at, count)],
                    send_sem=send_sem.at[r, step - 1], recv_sem=recv_sem.at[r, step - 1],
                    device_id={'seq': lax.rem(seq + step, N_SEQ)}, device_id_type=MESH))
                copies[-1].start()
            out[seq, at:at + count] = stage[at:at + count]
    for copy in copies:
        copy.wait()
    for copy in caches:
        copy.wait()


def project(tokens, w_query, w_key, w_value, k_cache, v_cache):
    batch, d_model = tokens.shape
    q_cols = w_query.shape[1] // (N_HEAD * N_SEQ)
    n_chunk = 8
    depth = d_model // n_chunk
    n_q = q_cols // LANES
    first = LANES + q_cols // 2
    second = q_cols - q_cols // 2
    return pl.pallas_call(
        functools.partial(project_kernel, n_chunk, 8),
        out_shape=[pltpu.VMEM((N_SEQ, n_q + 1, batch, LANES), BF16), pltpu.VMEM(k_cache.shape, BF16), pltpu.VMEM(k_cache.shape, BF16)],
        in_specs=[HBM] * 6,
        out_specs=[VMEM] * 3,
        scratch_shapes=[
            pltpu.VMEM((batch, d_model), BF16),
            pltpu.VMEM((n_chunk, depth, first), BF16),
            pltpu.VMEM((n_chunk, depth, second), BF16),
            pltpu.VMEM((batch, first), F32),
            pltpu.VMEM((batch, second), F32),
            pltpu.VMEM((n_q + 1, batch, LANES), BF16),
            pltpu.SemaphoreType.DMA((4, n_chunk)),
            pltpu.SemaphoreType.DMA((2, 8)),
            pltpu.SemaphoreType.DMA((2, N_SEQ - 1)),
            pltpu.SemaphoreType.DMA((2, N_SEQ - 1)),
        ],
        compiler_params=pltpu.CompilerParams(collective_id=0, has_side_effects=True, vmem_limit_bytes=18 * 2**20),
        name='project',
    )(*map(in_hbm, (tokens, w_query, w_key, w_value, k_cache, v_cache)))


def attend_kernel(n_chunk, shard_len, pos_ref, qkv_ref, k_in, v_in, k_out, v_out, mix_out, ml_out, kbuf, vbuf,
                  qf, kvf, store_sem):
    batch, rows = kbuf.shape[0], kbuf.shape[1]
    n_q = qkv_ref.shape[1] - 1
    n_rows = N_SEQ * n_q
    per = batch // n_chunk
    start = lax.axis_index('seq') * shard_len

    def store(hbm, buf, which, c):
        return pltpu.make_async_copy(buf.at[pl.ds(c * per, per)], hbm.at[pl.ds(c * per, per)], store_sem.at[which, c])

    for s in range(N_SEQ):
        for i in range(n_q):
            at = (s * n_q + i) * batch
            qf[at:at + batch, :] = qkv_ref[s, 1 + i].astype(F32)
        kvf[s * batch:(s + 1) * batch, :] = qkv_ref[s, 0].astype(F32)

    col = lax.broadcasted_iota(jnp.int32, (n_rows, rows), 1)
    row = lax.broadcasted_iota(jnp.int32, (n_rows, rows), 0)
    slot = jnp.where((col & 1) == row // (n_rows // 2), col >> 1, jnp.int32(1 << 30))
    win_row = lax.broadcasted_iota(jnp.int32, (16, LANES), 0)
    win_odd = (win_row & 1) == 1
    win_slot = win_row >> 1
    lane = lax.broadcasted_iota(jnp.int32, (n_rows, LANES), 1)

    def chunk(c, ml):
        for j in range(per):
            b = c * per + j
            pos = pos_ref[b] - start
            inside = jnp.logical_and(pos >= 0, pos < shard_len)
            slot_at = jnp.clip(pos, 0, shard_len - 1)
            base = pl.multiple_of((slot_at >> 3) * 16, 16)
            hit = win_slot == jnp.where(inside, slot_at & 7, -1)
            for buf, first in ((kbuf, 0), (vbuf, 2)):
                new = jnp.where(win_odd, kvf[pl.ds((first + 1) * batch + b, 1), :], kvf[pl.ds(first * batch + b, 1), :])
                old = buf[b, pl.ds(base, 16), :]
                buf[b, pl.ds(base, 16), :] = jnp.where(hit, new.astype(BF16), old)
        store(k_out, kbuf, 0, c).start()
        store(v_out, vbuf, 1, c).start()
        index = [c * per + j for j in range(per)]
        scores = []
        for b in index:
            q = qf[pl.ds(b, n_rows, stride=batch), :].astype(BF16)
            scores.append(lax.dot_general(q, kbuf[b], (((1,), (1,)), ((), ())), preferred_element_type=F32))
        weights = []
        for b, s in zip(index, scores):
            s = jnp.where(slot <= pos_ref[b] - start, s * LANES ** -0.5, -jnp.inf)
            m = jnp.max(s, axis=1, keepdims=True)
            w = jnp.exp(s - jnp.where(m == -jnp.inf, 0.0, m))
            l = jnp.sum(w, axis=1, keepdims=True)
            weights.append(w.astype(BF16))
            ml = jnp.where(lane == b, m, jnp.where(lane == batch + b, l, ml))
        for b, w in zip(index, weights):
            mix_out[pl.ds(b, n_rows, stride=batch), :] = jnp.dot(w, vbuf[b], preferred_element_type=F32)
        return ml

    ml = lax.fori_loop(0, n_chunk, chunk, jnp.zeros((n_rows, LANES), F32))
    ml_out[...] = jnp.zeros_like(ml_out)
    for s in range(N_SEQ):
        ml_out[s, 0:n_q, :] = ml[s * n_q:(s + 1) * n_q, :]
    for c in range(n_chunk):
        store(k_out, kbuf, 0, c).wait()
        store(v_out, vbuf, 1, c).wait()


def attend(positions, qkv, k_cache, v_cache, shard_len):
    batch, rows, _ = k_cache.shape
    n_rows = N_SEQ * (qkv.shape[1] - 1)
    n_chunk = 4
    cache = pltpu.HBM(k_cache.shape, BF16)
    held = pltpu.VMEM(k_cache.shape, BF16)
    return pl.pallas_call(
        functools.partial(attend_kernel, n_chunk, shard_len),
        out_shape=[cache, cache, pltpu.VMEM((n_rows * batch, LANES), F32), pltpu.VMEM((N_SEQ, 8, LANES), F32), held, held],
        in_specs=[SMEM, VMEM, VMEM, VMEM],
        out_specs=[HBM, HBM, VMEM, VMEM, VMEM, VMEM],
        input_output_aliases={2: 4, 3: 5},
        scratch_shapes=[
            pltpu.VMEM((n_rows * batch, LANES), F32),
            pltpu.VMEM((N_SEQ * batch, LANES), F32),
            pltpu.SemaphoreType.DMA((2, n_chunk)),
        ],
        compiler_params=pltpu.CompilerParams(vmem_limit_bytes=6 * 2**20),
        name='attend',
    )(positions, qkv, k_cache, v_cache)


def lane_table(rows):
    fill = jnp.zeros((LANES - 8 * len(rows), LANES), F32)
    return jnp.concatenate(list(rows) + [fill], axis=0).T


def merge(parts, batch):
    top = functools.reduce(jnp.maximum, parts)
    safe = jnp.where(top == -jnp.inf, 0.0, top)
    factors = [jnp.exp(p - safe) for p in parts]
    total = functools.reduce(jnp.add, [pltpu.roll(p, LANES - batch, 1) * e for p, e in zip(parts, factors)])
    return top, total, factors


def output_kernel(n_pass, mix, ml, wo_hbm, y, wo, pair_in, far_in, pair_ml, far_ml, far_give, far_give_ml, attn, give, own, core_in, y_in, z_in,
                  wo_sem, p_send, p_recv, f_send, f_recv, c_send, c_recv, y_send, y_recv, z_send, z_recv,
                  gz_send, gz_recv, gy_send, gy_recv, gc_send, gc_recv):
    head, seq = lax.axis_index('head'), lax.axis_index('seq')
    side, core = seq // 2, lax.rem(seq, 2)
    partner = side * 2 + (1 - core)
    across = (1 - side) * 2 + core
    diagonal = (1 - side) * 2 + (1 - core)
    n_q, batch = pair_in.shape[1], pair_in.shape[2]
    narrow = z_in.shape[3]
    wait_peers = entry_barrier((('seq', N_SEQ), ('head', N_HEAD)))

    def column(half, quarter, p, z=None):
        at = ((half * 2 + quarter) * n_pass + p) * N_HEAD * narrow
        return pl.multiple_of(at if z is None else at + z * narrow, narrow)

    def strip(z):
        return pl.ds(pl.multiple_of(z * narrow, narrow), narrow)

    def unit(near, p):
        return (1 if near else 0) * n_pass + p

    n_part = wo_sem.shape[0]
    part = wo.shape[0] // n_part
    wo_copies = [pltpu.make_async_copy(wo_hbm.at[pl.ds(n * part, part)], wo.at[pl.ds(n * part, part)], wo_sem.at[n]) for n in range(n_part)]
    for copy in wo_copies:
        copy.start()

    def remote(src, dst, send, recv, device):
        copy = pltpu.make_async_remote_copy(src_ref=src, dst_ref=dst, send_sem=send, recv_sem=recv, device_id=device, device_id_type=MESH)
        copy.start()
        return copy

    wait_peers()
    pair = []
    for n, to in enumerate((diagonal, partner)):
        pair.append(remote(ml.at[to], pair_ml.at[n], p_send.at[0, n], p_recv.at[0, n], {'seq': partner}))
        pair.append(remote(mix.at[pl.ds(to * n_q, n_q)], pair_in.at[n], p_send.at[1, n], p_recv.at[1, n], {'seq': partner}))
    pair[0].wait_recv()
    pair[1].wait_recv()
    top, total, factors = merge([ml[across], pair_ml[0]], batch)
    lane = lax.broadcasted_iota(jnp.int32, (8, LANES), 1)
    far_give_ml[...] = jnp.where(lane < batch, top, pltpu.roll(total, batch, 1))
    table = lane_table(factors)
    for i in range(n_q):
        far_give[i] = mix[across * n_q + i] * table[0:batch, i:i + 1] + pair_in[0, i] * table[0:batch, 8 + i:9 + i]
    far = [remote(far_give_ml, far_ml, f_send.at[0], f_recv.at[0], {'seq': across}),
           remote(far_give, far_in, f_send.at[1], f_recv.at[1], {'seq': across})]
    pair[2].wait_recv()
    pair[3].wait_recv()
    for copy in far:
        copy.wait_recv()
    _, total, factors = merge([ml[seq], pair_ml[1], far_ml[...]], batch)
    table = lane_table([e / total for e in factors])
    for i in range(n_q):
        value = mix[seq * n_q + i] * table[0:batch, i:i + 1]
        value += pair_in[1, i] * table[0:batch, 8 + i:9 + i]
        value += far_in[i] * table[0:batch, 16 + i:17 + i]
        attn[:, i * LANES:(i + 1) * LANES] = value.astype(BF16)
    sends = pair + far

    for copy in wo_copies:
        copy.wait()

    def partial(half, near, p):
        at = column(half, side if near else 1 - side, p)
        return jnp.dot(attn[...], wo[:, pl.ds(at, N_HEAD * narrow)], preferred_element_type=F32)

    def hand(near, p):
        u = unit(near, p)
        give[u] = partial(1 - core, near, p)
        c_copies[u] = remote(give.at[u], core_in.at[u], c_send.at[u], c_recv.at[u], {'seq': partner})

    def keep(near, p):
        u = unit(near, p)
        value = partial(core, near, p)
        c_copies[u].wait_recv()
        own[u] = value + core_in[u]

    c_copies, y_copies, z_copies = {}, {}, {}
    for p in range(n_pass):
        hand(False, p)
    for p in range(n_pass):
        keep(False, p)
        y_copies[p] = remote(own.at[unit(False, p)], y_in.at[p], y_send.at[p], y_recv.at[p], {'seq': across})
    for p in range(n_pass):
        hand(True, p)
    for p in range(n_pass):
        keep(True, p)

    def along(p):
        u = unit(True, p)
        y_copies[p].wait_recv()
        own[u] = own[u] + y_in[p]
        for step in (2, 1, 3):
            to = lax.rem(head + step, N_HEAD)
            z_copies[p, step] = remote(own.at[u, :, strip(to)], z_in.at[p, step - 1], z_send.at[p, step - 1], z_recv.at[p, step - 1],
                                       {'head': to})

    def spread(half, quarter, p, z, send, recv, device):
        at = y.at[:, pl.ds(column(half, quarter, p, z), narrow if z is not None else N_HEAD * narrow)]
        return remote(at, at, send, recv, device)

    gz, gy, gc = {}, {}, {}

    def finish(p):
        for step in (1, 3, 2):
            z_copies[p, step].wait_recv()
        value = own[unit(True, p), :, strip(head)] + z_in[p, 0] + z_in[p, 1] + z_in[p, 2]
        y[:, pl.ds(column(core, side, p, head), narrow)] = value.astype(BF16)
        for step in (2, 1, 3):
            gz[p, step] = spread(core, side, p, head, gz_send.at[p, step - 1], gz_recv.at[p, step - 1], {'head': lax.rem(head + step, N_HEAD)})

    def over(p):
        for step in (1, 3, 2):
            gz[p, step].wait_recv()
        gy[p] = spread(core, side, p, None, gy_send.at[p], gy_recv.at[p], {'seq': across})
        gc[p, 0] = spread(core, side, p, None, gc_send.at[p, 0], gc_recv.at[p, 0], {'seq': partner})

    def to_partner(p):
        gy[p].wait_recv()
        gc[p, 1] = spread(core, 1 - side, p, None, gc_send.at[p, 1], gc_recv.at[p, 1], {'seq': partner})

    stages = [(3 * p + at, n, p) for n, at in enumerate((0, 4.6, 9.3, 11.4)) for p in range(n_pass)]
    for _, n, p in sorted(stages):
        (along, finish, over, to_partner)[n](p)
    for copy in gc.values():
        copy.wait_recv()
    for group in (sends, *(g.values() for g in (c_copies, y_copies, z_copies, gz, gy, gc))):
        for copy in group:
            copy.wait_send()


def output(mix, ml, w_out):
    rows, d_out = w_out.shape
    n_q = rows // LANES
    batch = mix.shape[0] // (N_SEQ * n_q)
    n_pass = 4
    width = d_out // 16
    narrow = width // n_pass
    dma = pltpu.SemaphoreType.DMA
    block = pltpu.VMEM((n_q, batch, LANES), F32)
    return pl.pallas_call(
        functools.partial(output_kernel, n_pass),
        out_shape=pltpu.VMEM((batch, d_out), BF16),
        in_specs=[VMEM, VMEM, HBM],
        out_specs=VMEM,
        scratch_shapes=[
            pltpu.VMEM((rows, d_out), BF16),
            pltpu.VMEM((2, n_q, batch, LANES), F32),
            block,
            pltpu.VMEM((2, 8, LANES), F32),
            pltpu.VMEM((8, LANES), F32),
            block,
            pltpu.VMEM((8, LANES), F32),
            pltpu.VMEM((batch, rows), BF16),
            pltpu.VMEM((2 * n_pass, batch, width), F32),
            pltpu.VMEM((2 * n_pass, batch, width), F32),
            pltpu.VMEM((2 * n_pass, batch, width), F32),
            pltpu.VMEM((n_pass, batch, width), F32),
            pltpu.VMEM((n_pass, 3, batch, narrow), F32),
            dma((8,)),
            dma((2, 2)), dma((2, 2)), dma((2,)), dma((2,)),
            dma((2 * n_pass,)), dma((2 * n_pass,)), dma((n_pass,)), dma((n_pass,)), dma((n_pass, 3)), dma((n_pass, 3)),
            dma((n_pass, 3)), dma((n_pass, 3)), dma((n_pass,)), dma((n_pass,)), dma((n_pass, 2)), dma((n_pass, 2)),
        ],
        compiler_params=pltpu.CompilerParams(collective_id=1, has_side_effects=True, vmem_limit_bytes=24 * 2**20),
        name='output',
    )(mix.reshape(N_SEQ * n_q, batch, LANES), ml, in_hbm(w_out))


def solution(mesh):
    cache_spec = P('rep', 'seq', 'head', None)

    def local_step(tokens, w_query, w_key, w_value, w_out, k_cache, v_cache, positions):
        batch, shard_len, kv_local, head_dim = k_cache.shape
        flat = (batch, shard_len * kv_local, head_dim)
        qkv, k_held, v_held = project(tokens, w_query, w_key, w_value, k_cache.reshape(flat), v_cache.reshape(flat))
        k_new, v_new, mix, ml, _, _ = attend(positions, qkv, k_held, v_held, shard_len)
        y = output(mix, ml, w_out)
        return y, k_new.reshape(k_cache.shape), v_new.reshape(v_cache.shape)

    return jax.shard_map(
        local_step,
        mesh=mesh,
        in_specs=(P('rep', None), P(), P(), P(), P(('head', 'seq'), None), cache_spec, cache_spec, P('rep')),
        out_specs=(P('rep', None), cache_spec, cache_spec),
        check_vma=False,
    )
```

```python
import functools

import jax
import jax.numpy as jnp
from jax import lax
from jax.experimental import pallas as pl
from jax.experimental.pallas import tpu as pltpu
from jax.sharding import PartitionSpec as P

MESH = pl.DeviceIdType.MESH
HBM = pl.BlockSpec(memory_space=pltpu.HBM)
VMEM = pl.BlockSpec(memory_space=pltpu.VMEM)
SMEM = pl.BlockSpec(memory_space=pltpu.SMEM)
N_SEQ = 4
N_HEAD = 4
LANES = 128
F32 = jnp.float32
BF16 = jnp.bfloat16


def in_hbm(x):
    return pltpu.with_memory_space_constraint(x, pltpu.HBM)


def entry_barrier(axes):
    sem = pltpu.get_barrier_semaphore()
    count = 0
    for axis, size in axes:
        me = lax.axis_index(axis)
        for step in range(1, size):
            pl.semaphore_signal(sem, inc=1, device_id={axis: lax.rem(me + step, size)}, device_id_type=MESH)
            count += 1
    return lambda: pl.semaphore_wait(sem, count)


def project_kernel(n_chunk, ahead, tok_hbm, wq_hbm, wk_hbm, wv_hbm, k_hbm, v_hbm, out, kbuf, vbuf, tok, w_first, w_second,
                   acc_first, acc_second, stage, load_sem, cache_sem, send_sem, recv_sem):
    head, seq = lax.axis_index('head'), lax.axis_index('seq')
    depth = w_first.shape[1]
    batch = tok.shape[0]
    wait_peers = entry_barrier((('seq', N_SEQ),))

    second = w_second.shape[2]
    first = w_first.shape[2] - LANES
    q_at = (head * N_SEQ + seq) * (first + second)
    kv_at = pl.multiple_of((head * 2 + lax.rem(seq, 2)) * LANES, LANES)

    def tok_copy(c):
        return pltpu.make_async_copy(tok_hbm.at[:, pl.ds(c * depth, depth)], tok.at[:, pl.ds(c * depth, depth)], load_sem.at[0, c])

    def kv_copy(src, c):
        return pltpu.make_async_copy(src.at[pl.ds(c * depth, depth), pl.ds(kv_at, LANES)], w_first.at[c, :, pl.ds(0, LANES)],
                                     load_sem.at[1, c])

    def q_copy(r, c):
        rows = pl.ds(c * depth, depth)
        if r == 0:
            at = pl.multiple_of(q_at, LANES)
            return pltpu.make_async_copy(wq_hbm.at[rows, pl.ds(at, first)], w_first.at[c, :, pl.ds(LANES, first)], load_sem.at[2, c])
        at = pl.multiple_of(q_at + first, LANES)
        return pltpu.make_async_copy(wq_hbm.at[rows, pl.ds(at, second)], w_second.at[c], load_sem.at[3, c])

    def start(r, c):
        q_copy(r, c).start()
        if r == 0:
            tok_copy(c).start()

            @pl.when(seq < 2)
            def _():
                kv_copy(wk_hbm, c).start()

            @pl.when(seq >= 2)
            def _():
                kv_copy(wv_hbm, c).start()

    caches = []
    for g in range(8):
        span = pl.ds(g * (batch // 8), batch // 8)
        caches.append(pltpu.make_async_copy(k_hbm.at[span], kbuf.at[span], cache_sem.at[0, g]))
        caches.append(pltpu.make_async_copy(v_hbm.at[span], vbuf.at[span], cache_sem.at[1, g]))
    share = len(caches) // ahead
    held = 0

    turns = [(r, c) for r in range(2) for c in range(n_chunk)]
    copies = []
    for r, c in turns[:ahead]:
        start(r, c)
    for n, (r, c) in enumerate(turns):
        if n + ahead < len(turns):
            start(*turns[n + ahead])
        else:
            for copy in caches[held:held + share]:
                copy.start()
            held += share
        q_copy(r, c).wait()
        if r == 0:
            tok_copy(c).wait()
            kv_copy(wk_hbm, c).wait()
        acc, w = ((acc_first, w_first), (acc_second, w_second))[r]
        part = jnp.dot(tok[:, c * depth:(c + 1) * depth], w[c], preferred_element_type=F32)
        if c == 0:
            acc[...] = part
        else:
            acc[...] += part
        if c == n_chunk - 1:
            at, count = (0, acc.shape[1] // LANES) if r == 0 else (w_first.shape[2] // LANES, acc.shape[1] // LANES)
            for i in range(count):
                stage[at + i] = acc[:, i * LANES:(i + 1) * LANES].astype(BF16)
            if r == 0:
                wait_peers()
            for step in (2, 1, 3):
                copies.append(pltpu.make_async_remote_copy(
                    src_ref=stage.at[pl.ds(at, count)], dst_ref=out.at[seq, pl.ds(at, count)],
                    send_sem=send_sem.at[r, step - 1], recv_sem=recv_sem.at[r, step - 1],
                    device_id={'seq': lax.rem(seq + step, N_SEQ)}, device_id_type=MESH))
                copies[-1].start()
            out[seq, at:at + count] = stage[at:at + count]
    for copy in copies:
        copy.wait()
    for copy in caches:
        copy.wait()


def project(tokens, w_query, w_key, w_value, k_cache, v_cache):
    batch, d_model = tokens.shape
    q_cols = w_query.shape[1] // (N_HEAD * N_SEQ)
    n_chunk = 8
    depth = d_model // n_chunk
    n_q = q_cols // LANES
    first = LANES + q_cols // 2
    second = q_cols - q_cols // 2
    return pl.pallas_call(
        functools.partial(project_kernel, n_chunk, 8),
        out_shape=[pltpu.VMEM((N_SEQ, n_q + 1, batch, LANES), BF16), pltpu.VMEM(k_cache.shape, BF16), pltpu.VMEM(k_cache.shape, BF16)],
        in_specs=[HBM] * 6,
        out_specs=[VMEM] * 3,
        scratch_shapes=[
            pltpu.VMEM((batch, d_model), BF16),
            pltpu.VMEM((n_chunk, depth, first), BF16),
            pltpu.VMEM((n_chunk, depth, second), BF16),
            pltpu.VMEM((batch, first), F32),
            pltpu.VMEM((batch, second), F32),
            pltpu.VMEM((n_q + 1, batch, LANES), BF16),
            pltpu.SemaphoreType.DMA((4, n_chunk)),
            pltpu.SemaphoreType.DMA((2, 8)),
            pltpu.SemaphoreType.DMA((2, N_SEQ - 1)),
            pltpu.SemaphoreType.DMA((2, N_SEQ - 1)),
        ],
        compiler_params=pltpu.CompilerParams(collective_id=0, has_side_effects=True, vmem_limit_bytes=18 * 2**20),
        name='project',
    )(*map(in_hbm, (tokens, w_query, w_key, w_value, k_cache, v_cache)))


def attend_kernel(n_chunk, shard_len, pos_ref, qkv_ref, k_in, v_in, k_out, v_out, mix_out, ml_out, kbuf, vbuf,
                  qf, kvf, store_sem):
    batch, rows = kbuf.shape[0], kbuf.shape[1]
    n_q = qkv_ref.shape[1] - 1
    n_rows = N_SEQ * n_q
    per = batch // n_chunk
    start = lax.axis_index('seq') * shard_len

    def store(hbm, buf, which, c):
        return pltpu.make_async_copy(buf.at[pl.ds(c * per, per)], hbm.at[pl.ds(c * per, per)], store_sem.at[which, c])

    for s in range(N_SEQ):
        for i in range(n_q):
            at = (s * n_q + i) * batch
            qf[at:at + batch, :] = qkv_ref[s, 1 + i].astype(F32)
        kvf[s * batch:(s + 1) * batch, :] = qkv_ref[s, 0].astype(F32)

    col = lax.broadcasted_iota(jnp.int32, (n_rows, rows), 1)
    row = lax.broadcasted_iota(jnp.int32, (n_rows, rows), 0)
    slot = jnp.where((col & 1) == row // (n_rows // 2), col >> 1, jnp.int32(1 << 30))
    win_row = lax.broadcasted_iota(jnp.int32, (16, LANES), 0)
    win_odd = (win_row & 1) == 1
    win_slot = win_row >> 1
    lane = lax.broadcasted_iota(jnp.int32, (n_rows, LANES), 1)

    def chunk(c, ml):
        for j in range(per):
            b = c * per + j
            pos = pos_ref[b] - start
            inside = jnp.logical_and(pos >= 0, pos < shard_len)
            slot_at = jnp.clip(pos, 0, shard_len - 1)
            base = pl.multiple_of((slot_at >> 3) * 16, 16)
            hit = win_slot == jnp.where(inside, slot_at & 7, -1)
            for buf, first in ((kbuf, 0), (vbuf, 2)):
                new = jnp.where(win_odd, kvf[pl.ds((first + 1) * batch + b, 1), :], kvf[pl.ds(first * batch + b, 1), :])
                old = buf[b, pl.ds(base, 16), :]
                buf[b, pl.ds(base, 16), :] = jnp.where(hit, new.astype(BF16), old)
        store(k_out, kbuf, 0, c).start()
        store(v_out, vbuf, 1, c).start()
        index = [c * per + j for j in range(per)]
        scores = []
        for b in index:
            q = qf[pl.ds(b, n_rows, stride=batch), :].astype(BF16)
            scores.append(lax.dot_general(q, kbuf[b], (((1,), (1,)), ((), ())), preferred_element_type=F32))
        weights = []
        for b, s in zip(index, scores):
            s = jnp.where(slot <= pos_ref[b] - start, s * LANES ** -0.5, -jnp.inf)
            m = jnp.max(s, axis=1, keepdims=True)
            w = jnp.exp(s - jnp.where(m == -jnp.inf, 0.0, m))
            l = jnp.sum(w, axis=1, keepdims=True)
            weights.append(w.astype(BF16))
            ml = jnp.where(lane == b, m, jnp.where(lane == batch + b, l, ml))
        for b, w in zip(index, weights):
            mix_out[pl.ds(b, n_rows, stride=batch), :] = jnp.dot(w, vbuf[b], preferred_element_type=F32)
        return ml

    ml = lax.fori_loop(0, n_chunk, chunk, jnp.zeros((n_rows, LANES), F32))
    ml_out[...] = jnp.zeros_like(ml_out)
    for s in range(N_SEQ):
        ml_out[s, 0:n_q, :] = ml[s * n_q:(s + 1) * n_q, :]
    for c in range(n_chunk):
        store(k_out, kbuf, 0, c).wait()
        store(v_out, vbuf, 1, c).wait()


def attend(positions, qkv, k_cache, v_cache, shard_len):
    batch, rows, _ = k_cache.shape
    n_rows = N_SEQ * (qkv.shape[1] - 1)
    n_chunk = 4
    cache = pltpu.HBM(k_cache.shape, BF16)
    held = pltpu.VMEM(k_cache.shape, BF16)
    return pl.pallas_call(
        functools.partial(attend_kernel, n_chunk, shard_len),
        out_shape=[cache, cache, pltpu.VMEM((n_rows * batch, LANES), F32), pltpu.VMEM((N_SEQ, 8, LANES), F32), held, held],
        in_specs=[SMEM, VMEM, VMEM, VMEM],
        out_specs=[HBM, HBM, VMEM, VMEM, VMEM, VMEM],
        input_output_aliases={2: 4, 3: 5},
        scratch_shapes=[
            pltpu.VMEM((n_rows * batch, LANES), F32),
            pltpu.VMEM((N_SEQ * batch, LANES), F32),
            pltpu.SemaphoreType.DMA((2, n_chunk)),
        ],
        compiler_params=pltpu.CompilerParams(vmem_limit_bytes=6 * 2**20),
        name='attend',
    )(positions, qkv, k_cache, v_cache)


def lane_table(rows):
    fill = jnp.zeros((LANES - 8 * len(rows), LANES), F32)
    return jnp.concatenate(list(rows) + [fill], axis=0).T


def merge(parts, batch):
    top = functools.reduce(jnp.maximum, parts)
    safe = jnp.where(top == -jnp.inf, 0.0, top)
    factors = [jnp.exp(p - safe) for p in parts]
    total = functools.reduce(jnp.add, [pltpu.roll(p, LANES - batch, 1) * e for p, e in zip(parts, factors)])
    return top, total, factors


def output_kernel(n_pass, mix, ml, wo_hbm, y, wo, pair_in, far_in, pair_ml, far_ml, far_give, far_give_ml, attn, give, own, core_in, y_in, z_in, whole,
                  wo_sem, p_send, p_recv, f_send, f_recv, c_send, c_recv, y_send, y_recv, z_send, z_recv,
                  gz_send, gz_recv, gy_send, gy_recv, gc_send, gc_recv):
    head, seq = lax.axis_index('head'), lax.axis_index('seq')
    side, core = seq // 2, lax.rem(seq, 2)
    partner = side * 2 + (1 - core)
    across = (1 - side) * 2 + core
    diagonal = (1 - side) * 2 + (1 - core)
    n_q, batch = pair_in.shape[1], pair_in.shape[2]
    narrow = z_in.shape[3]
    wait_peers = entry_barrier((('seq', N_SEQ), ('head', N_HEAD)))

    def place(half, quarter, p):
        return (half * 2 + quarter) * n_pass + p

    def unit(near, p):
        return (1 if near else 0) * n_pass + p

    n_part = wo_sem.shape[0]
    part = wo.shape[0] // n_part
    wo_copies = [pltpu.make_async_copy(wo_hbm.at[pl.ds(n * part, part)], wo.at[pl.ds(n * part, part)], wo_sem.at[n]) for n in range(n_part)]
    for copy in wo_copies:
        copy.start()

    def remote(src, dst, send, recv, device):
        copy = pltpu.make_async_remote_copy(src_ref=src, dst_ref=dst, send_sem=send, recv_sem=recv, device_id=device, device_id_type=MESH)
        copy.start()
        return copy

    wait_peers()
    pair = []
    for n, to in enumerate((diagonal, partner)):
        pair.append(remote(ml.at[to], pair_ml.at[n], p_send.at[0, n], p_recv.at[0, n], {'seq': partner}))
        pair.append(remote(mix.at[pl.ds(to * n_q, n_q)], pair_in.at[n], p_send.at[1, n], p_recv.at[1, n], {'seq': partner}))
    pair[0].wait_recv()
    pair[1].wait_recv()
    top, total, factors = merge([ml[across], pair_ml[0]], batch)
    lane = lax.broadcasted_iota(jnp.int32, (8, LANES), 1)
    far_give_ml[...] = jnp.where(lane < batch, top, pltpu.roll(total, batch, 1))
    table = lane_table(factors)
    for i in range(n_q):
        far_give[i] = mix[across * n_q + i] * table[0:batch, i:i + 1] + pair_in[0, i] * table[0:batch, 8 + i:9 + i]
    far = [remote(far_give_ml, far_ml, f_send.at[0], f_recv.at[0], {'seq': across}),
           remote(far_give, far_in, f_send.at[1], f_recv.at[1], {'seq': across})]
    pair[2].wait_recv()
    pair[3].wait_recv()
    for copy in far:
        copy.wait_recv()
    _, total, factors = merge([ml[seq], pair_ml[1], far_ml[...]], batch)
    table = lane_table([e / total for e in factors])
    for i in range(n_q):
        value = mix[seq * n_q + i] * table[0:batch, i:i + 1]
        value += pair_in[1, i] * table[0:batch, 8 + i:9 + i]
        value += far_in[i] * table[0:batch, 16 + i:17 + i]
        attn[:, i * LANES:(i + 1) * LANES] = value.astype(BF16)
    sends = pair + far

    for copy in wo_copies:
        copy.wait()

    def partial(half, near, p):
        at = pl.multiple_of(place(half, side if near else 1 - side, p) * N_HEAD * narrow, narrow)
        value = jnp.dot(attn[...], wo[:, pl.ds(at, N_HEAD * narrow)], preferred_element_type=F32)
        return [value[:, z * narrow:(z + 1) * narrow] for z in range(N_HEAD)]

    def hand(near, p):
        u = unit(near, p)
        for z, value in enumerate(partial(1 - core, near, p)):
            give[u, z] = value
        c_copies[u] = remote(give.at[u], core_in.at[u], c_send.at[u], c_recv.at[u], {'seq': partner})

    def keep(near, p):
        u = unit(near, p)
        values = partial(core, near, p)
        c_copies[u].wait_recv()
        for z, value in enumerate(values):
            own[u, z] = value + core_in[u, z]

    c_copies, y_copies, z_copies = {}, {}, {}
    for p in range(n_pass):
        hand(False, p)
    for p in range(n_pass):
        keep(False, p)
        y_copies[p] = remote(own.at[unit(False, p)], y_in.at[p], y_send.at[p], y_recv.at[p], {'seq': across})
    for p in range(n_pass):
        hand(True, p)
    for p in range(n_pass):
        keep(True, p)

    def along(p):
        u = unit(True, p)
        y_copies[p].wait_recv()
        own[u] = own[u] + y_in[p]
        for step in (2, 1, 3):
            to = lax.rem(head + step, N_HEAD)
            z_copies[p, step] = remote(own.at[u, to], z_in.at[p, step - 1], z_send.at[p, step - 1], z_recv.at[p, step - 1],
                                       {'head': to})

    def spread(at, send, recv, device):
        return remote(at, at, send, recv, device)

    gz, gy, gc = {}, {}, {}

    def finish(p):
        for step in (1, 3, 2):
            z_copies[p, step].wait_recv()
        at = place(core, side, p)
        whole[at, head] = (own[unit(True, p), head] + z_in[p, 0] + z_in[p, 1] + z_in[p, 2]).astype(BF16)
        for step in (2, 1, 3):
            gz[p, step] = spread(whole.at[at, head], gz_send.at[p, step - 1], gz_recv.at[p, step - 1], {'head': lax.rem(head + step, N_HEAD)})

    def over(p):
        for step in (1, 3, 2):
            gz[p, step].wait_recv()
        at = whole.at[place(core, side, p)]
        gy[p] = spread(at, gy_send.at[p], gy_recv.at[p], {'seq': across})
        gc[p, 0] = spread(at, gc_send.at[p, 0], gc_recv.at[p, 0], {'seq': partner})

    def to_partner(p):
        gy[p].wait_recv()
        gc[p, 1] = spread(whole.at[place(core, 1 - side, p)], gc_send.at[p, 1], gc_recv.at[p, 1], {'seq': partner})

    stages = [(3 * p + at, n, p) for n, at in enumerate((0, 4.6, 9.3, 11.4)) for p in range(n_pass)]
    for _, n, p in sorted(stages):
        (along, finish, over, to_partner)[n](p)
    for copy in gc.values():
        copy.wait_recv()
    for u in range(whole.shape[0]):
        for z in range(N_HEAD):
            y[:, (u * N_HEAD + z) * narrow:(u * N_HEAD + z + 1) * narrow] = whole[u, z]
    for group in (sends, *(g.values() for g in (c_copies, y_copies, z_copies, gz, gy, gc))):
        for copy in group:
            copy.wait_send()


def output(mix, ml, w_out):
    rows, d_out = w_out.shape
    n_q = rows // LANES
    batch = mix.shape[0] // (N_SEQ * n_q)
    n_pass = 4
    width = d_out // 16
    narrow = width // n_pass
    dma = pltpu.SemaphoreType.DMA
    block = pltpu.VMEM((n_q, batch, LANES), F32)
    return pl.pallas_call(
        functools.partial(output_kernel, n_pass),
        out_shape=pltpu.VMEM((batch, d_out), BF16),
        in_specs=[VMEM, VMEM, HBM],
        out_specs=VMEM,
        scratch_shapes=[
            pltpu.VMEM((rows, d_out), BF16),
            pltpu.VMEM((2, n_q, batch, LANES), F32),
            block,
            pltpu.VMEM((2, 8, LANES), F32),
            pltpu.VMEM((8, LANES), F32),
            block,
            pltpu.VMEM((8, LANES), F32),
            pltpu.VMEM((batch, rows), BF16),
            pltpu.VMEM((2 * n_pass, N_HEAD, batch, narrow), F32),
            pltpu.VMEM((2 * n_pass, N_HEAD, batch, narrow), F32),
            pltpu.VMEM((2 * n_pass, N_HEAD, batch, narrow), F32),
            pltpu.VMEM((n_pass, N_HEAD, batch, narrow), F32),
            pltpu.VMEM((n_pass, 3, batch, narrow), F32),
            pltpu.VMEM((4 * n_pass, N_HEAD, batch, narrow), BF16),
            dma((8,)),
            dma((2, 2)), dma((2, 2)), dma((2,)), dma((2,)),
            dma((2 * n_pass,)), dma((2 * n_pass,)), dma((n_pass,)), dma((n_pass,)), dma((n_pass, 3)), dma((n_pass, 3)),
            dma((n_pass, 3)), dma((n_pass, 3)), dma((n_pass,)), dma((n_pass,)), dma((n_pass, 2)), dma((n_pass, 2)),
        ],
        compiler_params=pltpu.CompilerParams(collective_id=1, has_side_effects=True, vmem_limit_bytes=24 * 2**20),
        name='output',
    )(mix.reshape(N_SEQ * n_q, batch, LANES), ml, in_hbm(w_out))


def solution(mesh):
    cache_spec = P('rep', 'seq', 'head', None)

    def local_step(tokens, w_query, w_key, w_value, w_out, k_cache, v_cache, positions):
        batch, shard_len, kv_local, head_dim = k_cache.shape
        flat = (batch, shard_len * kv_local, head_dim)
        qkv, k_held, v_held = project(tokens, w_query, w_key, w_value, k_cache.reshape(flat), v_cache.reshape(flat))
        k_new, v_new, mix, ml, _, _ = attend(positions, qkv, k_held, v_held, shard_len)
        y = output(mix, ml, w_out)
        return y, k_new.reshape(k_cache.shape), v_new.reshape(v_cache.shape)

    return jax.shard_map(
        local_step,
        mesh=mesh,
        in_specs=(P('rep', None), P(), P(), P(), P(('head', 'seq'), None), cache_spec, cache_spec, P('rep')),
        out_specs=(P('rep', None), cache_spec, cache_spec),
        check_vma=False,
    )
```
